512 devices in a mesh: groups: 2 (over y), seq: 32 (over z), tp: 8 (over x, core).
Axes of the slice: x: 4, y: 2, z: 32, core: 2. Of those that a mesh axis runs over, the one named last changes fastest.
The devices are a block of a 4x8x32 slice.
Arguments:
- q_prefill: bfloat16 [16384, 4096], P(('groups', 'seq'), 'tp'), parts along dimension 0, may hold values from -8 to 8
- k_prefill: bfloat16 [16384, 1024], P(('groups', 'seq'), 'tp'), parts along dimension 0, may hold values from -8 to 8
- v_prefill: bfloat16 [16384, 1024], P(('groups', 'seq'), 'tp'), parts along dimension 0, may hold values from -6 to 6
- pair_lengths: int32 [16], P('groups'), parts along dimension 0, may hold values from 1 to 5120, 8192 in all
- q_decode: bfloat16 [8, 4096], P('groups', 'tp'), parts along dimension 0, may hold values from -8 to 8
- cache_k: bfloat16 [8, 2048, 1024], P('groups', 'seq', 'tp'), parts along dimension 0, may hold values from -8 to 8
- cache_v: bfloat16 [8, 2048, 1024], P('groups', 'seq', 'tp'), parts along dimension 0, may hold values from -6 to 6
- cache_lengths: int32 [8], P('groups'), parts along dimension 0, may hold values from 256 to 2048
- stream: bfloat16 [24, 8192], P('groups', 'seq'), parts along dimension 0, may hold values from -40 to 40
- out_weight: bfloat16 [4096, 8192], P('tp', 'seq'), may hold values from -0.09375 to 0.09375
- norm_gain: bfloat16 [8192], P('seq'), may hold values from 0.099609375 to 1.8984375
- vocab_table: bfloat16 [64128, 8192], P('tp', 'seq'), may hold values from -0.0625 to 0.0625
- verdict_ids: int32 [24, 2], P('groups'), parts along dimension 0, may hold values from 0 to 64127
Outputs:
- attended: bfloat16 [16384, 4096], P(('groups', 'seq'), 'tp'), parts along dimension 0
- verdict_hidden: bfloat16 [24, 8192], P('groups', 'seq'), parts along dimension 0
- win: float32 [24], P('groups'), parts along dimension 0
The draws below stay inside these ranges and needn't reach their ends.
There are 2 independent parts, one for each index of `groups`. The reference program is written for one: setup_inputs(seed, part) draws one part's arguments, and reference() takes and returns one part's arrays. A program takes and returns all parts, laid end to end along the dimension named above; an argument that names none is the same for every part. Nothing has to cross between parts.
Inputs may be any that keep to these rules, and one draw needn't show every extreme that they name: `pair_lengths`: the segments lie end to end from position 0 and each is at most 5120 long.
All inputs are finite; a program needn't handle non-finite values.
Results may differ from the reference program's by a relative error of at most 0.008.
Values may be sent and summed in bfloat16 or wider, within the bound.
No kernel may reach another device: no remote copies, remote signals or barrier semaphores. Data moves between devices by JAX's collectives and lax.ppermute only.
A program may use at most 64 MiB of HBM per device.

```python
import math
import jax
import jax.numpy as jnp
import numpy as np
from jax import lax

D = 8192
H = 32
KVH = 8
HD = 128
VOCAB = 64128
TOK_DEV = 256
PAIRS = 8
PROMPTS = 4
STRETCH = 8192
MOST = 5120
CACHE = 2048
ROWS = 12


def base_field(key, shape):
    return jnp.clip(1.75 * jax.random.normal(key, shape, jnp.float32), -8.0, 8.0)


def marked_pair(sign_table, amplitudes):
    vectors = sign_table * amplitudes[:, None]
    shrink = 2.0 * math.sqrt(HD) / amplitudes
    second = vectors.at[:, 0].set(sign_table[:, 0] * (amplitudes - shrink))
    return (vectors, second)


def prefill_marks(key):
    base = jax.random.fold_in(key, 7001)
    key_pos, key_head, key_sign = jax.random.split(base, 3)
    positions = jax.random.randint(key_pos, (3,), 1, STRETCH)
    head_picks = jax.random.randint(key_head, (3,), 0, H)
    sign_table = (2 * jax.random.randint(key_sign, (3, HD), 0, 2) - 1).astype(jnp.float32)
    vectors, second = marked_pair(sign_table, jnp.array([7.5, 7.0, 6.5], jnp.float32))
    return (positions, head_picks, vectors, second)


def decode_marks(key):
    base = jax.random.fold_in(key, 7002)
    key_head, key_sign = jax.random.split(base, 2)
    head_picks = jax.random.randint(key_head, (PROMPTS,), 0, H)
    sign_table = (2 * jax.random.randint(key_sign, (PROMPTS, HD), 0, 2) - 1).astype(jnp.float32)
    amplitudes = jnp.array([7.5, 7.0, 6.5], jnp.float32)[jnp.arange(PROMPTS) % 3]
    vectors, second = marked_pair(sign_table, amplitudes)
    return (head_picks, vectors, second)


def draw_q_prefill(key, part):
    field = base_field(jax.random.fold_in(key, 1), (STRETCH, H * HD))
    positions, head_picks, vectors, second = prefill_marks(key)
    columns = head_picks[:, None] * HD + jnp.arange(HD)[None, :]
    field = field.at[positions[:, None], columns].set(vectors)
    return field.astype(jnp.bfloat16)


def draw_k_prefill(key, part):
    field = base_field(jax.random.fold_in(key, 2), (STRETCH, KVH * HD))
    positions, head_picks, vectors, second = prefill_marks(key)
    columns = (head_picks // (H // KVH))[:, None] * HD + jnp.arange(HD)[None, :]
    field = field.at[positions[:, None], columns].set(vectors)
    field = field.at[positions[:, None] - 1, columns].set(second)
    return field.astype(jnp.bfloat16)


def draw_q_decode(key, part):
    field = base_field(jax.random.fold_in(key, 3), (PROMPTS, H * HD))
    head_picks, vectors, second = decode_marks(key)
    columns = head_picks[:, None] * HD + jnp.arange(HD)[None, :]
    prompt_rows = jnp.arange(PROMPTS)[:, None]
    field = field.at[prompt_rows, columns].set(vectors)
    return field.astype(jnp.bfloat16)


def draw_cache_k(key, part):
    field = base_field(jax.random.fold_in(key, 4), (PROMPTS, CACHE, KVH * HD))
    head_picks, vectors, second = decode_marks(key)
    columns = (head_picks // (H // KVH))[:, None] * HD + jnp.arange(HD)[None, :]
    prompt_rows = jnp.arange(PROMPTS)[:, None]
    field = field.at[prompt_rows, 0, columns].set(vectors)
    field = field.at[prompt_rows, 1, columns].set(second)
    return field.astype(jnp.bfloat16)


def draw_stream(key, part):
    key_rows, key_noise = jax.random.split(jax.random.fold_in(key, 5), 2)
    row_scale = jnp.exp(jax.random.uniform(key_rows, (ROWS, 1), jnp.float32, math.log(0.3), math.log(3.0)))
    column_ramp = jnp.arange(D, dtype=jnp.float32)[None, :] / D
    noise_part = jnp.clip(jax.random.normal(key_noise, (ROWS, D), jnp.float32), -6.0, 6.0)
    column_scale = math.sqrt(3.0) ** column_ramp
    return (noise_part * row_scale * column_scale).astype(jnp.bfloat16)


def set_ends(drawn, key, low, high):
    longest = drawn.shape.index(max(drawn.shape))
    spots = []
    for shift in (0, 1):
        where = [jax.random.randint(jax.random.fold_in(key, axis), (), 0, length) for axis, length in enumerate(drawn.shape)]
        where[longest] = (where[longest] + shift) % drawn.shape[longest]
        spots.append(tuple(where))
    return drawn.at[spots[0]].set(low).at[spots[1]].set(high)


def shard_levels(stream_key, extent, pieces, least, high):
    factor_of, own = 1.0, jax.random.fold_in(stream_key, 6)
    for axis_at, blocks in pieces:
        steps = jnp.exp(jax.random.uniform(jax.random.fold_in(own, axis_at), (blocks,), jnp.float32, least / len(pieces), high / len(pieces)))
        factor_of = factor_of * jnp.repeat(steps, extent[axis_at] // blocks).reshape([-1 if axis == axis_at else 1 for axis in range(len(extent))])
    return factor_of


def length_profile(amount, total, most, lean):
    portions = [(1 << 20) // math.isqrt(standing ** lean) + 1 for standing in range(2, amount + 1)]
    spare, counts = total - most - (amount - 1), [1] * (amount - 1)
    while spare > 0:
        free = [i for i in range(amount - 1) if counts[i] < most]
        pool, budget = sum([portions[i] for i in free]), spare
        for i in free:
            more = min(most - counts[i], max(1, budget * portions[i] // pool), spare)
            counts[i] = counts[i] + more
            spare = spare - more
    return np.array([most] + counts)


def ragged_sizes(rng, amount, total, bound, slope):
    if amount == 2:
        one = jax.random.randint(rng, (), max(1, total - bound), min(bound, total - 1) + 1)
        return jnp.stack([one, total - one])
    lengths = jnp.asarray(length_profile(amount, total, bound, slope), jnp.int32)
    twos = (amount - 1) // 2
    giver, taker = lengths[1:1 + 2 * twos:2], lengths[2:2 + 2 * twos:2]
    slack = jnp.minimum(giver - 1, bound - taker)
    moved = jax.random.randint(jax.random.fold_in(rng, 1), (twos,), 0, 1 << 20) % (slack + 1)
    lengths = lengths.at[1:1 + 2 * twos:2].set(giver - moved).at[2:2 + 2 * twos:2].set(taker + moved)
    return lengths[jax.random.permutation(jax.random.fold_in(rng, 2), amount)]


def gaussian(rng, extent, scale, limit, cuts=(), held_as=jnp.bfloat16):
    loudness = shard_levels(rng, extent, cuts, -0.22, 0.18) if cuts else 1.0
    values = jax.random.normal(rng, extent, jnp.float32) * scale * loudness
    return jnp.minimum(jnp.maximum(values, -limit), limit).astype(held_as)


def setup_inputs(seed: int = 0, part: int = 0) -> dict:
    seeds = jax.random.split(jax.random.key(seed), 14)
    part_keys = jax.random.split(jax.random.fold_in(seeds[13], part), 14)
    return {
        "q_prefill": draw_q_prefill(jax.random.fold_in(jax.random.fold_in(seeds[13], part), 71), part),
        "k_prefill": draw_k_prefill(jax.random.fold_in(jax.random.fold_in(seeds[13], part), 71), part),
        "v_prefill": gaussian(part_keys[2], (STRETCH, KVH * HD), 1.0, 6.0, ((0, 32), (1, 8))),
        "pair_lengths": ragged_sizes(part_keys[3], PAIRS, STRETCH, MOST, 2).astype(jnp.int32),
        "q_decode": draw_q_decode(jax.random.fold_in(jax.random.fold_in(seeds[13], part), 71), part),
        "cache_k": draw_cache_k(jax.random.fold_in(jax.random.fold_in(seeds[13], part), 71), part),
        "cache_v": gaussian(part_keys[6], (PROMPTS, CACHE, KVH * HD), 1.0, 6.0, ((1, 32), (2, 8))),
        "cache_lengths": set_ends(jax.random.randint(part_keys[7], (PROMPTS,), CACHE // 8, CACHE + 1), jax.random.fold_in(part_keys[7], 1), CACHE // 8, CACHE).astype(jnp.int32),
        "stream": draw_stream(jax.random.fold_in(jax.random.fold_in(seeds[13], part), 71), part),
        "out_weight": gaussian(seeds[9], (H * HD, D), (H * HD) ** -0.5, 0.09375, ((0, 8), (1, 32))),
        "norm_gain": jnp.clip(1.0 + 0.18 * jax.random.normal(seeds[10], (D,), jnp.float32), 0.099609375, 1.8984375).astype(jnp.bfloat16),
        "vocab_table": gaussian(seeds[11], (VOCAB, D), D ** -0.5, 0.0625, ((0, 8), (1, 32))),
        "verdict_ids": set_ends(jax.random.randint(part_keys[12], (ROWS, 2), 0, VOCAB), jax.random.fold_in(part_keys[12], 1), 0, VOCAB - 1).astype(jnp.int32),
    }


masked_score = -1e+30
norm_eps = 1e-05

def segment_of(positions, pair_ends):
    return lax.optimization_barrier(jnp.sum((pair_ends[None, :] <= positions[:, None]).astype(jnp.int32), axis=1))

def reference(q_prefill, k_prefill, v_prefill, pair_lengths, q_decode, cache_k, cache_v, cache_lengths, stream, out_weight, norm_gain, vocab_table, verdict_ids):
    group_size = H // KVH
    score_scale = 1.0 / HD ** 0.5
    pair_ends = jnp.cumsum(pair_lengths).astype(jnp.int32)
    all_pos = jnp.arange(STRETCH, dtype=jnp.int32)
    all_seg = segment_of(all_pos, pair_ends)
    keys_all = k_prefill.reshape(STRETCH, KVH, HD).astype(jnp.float32)
    values_all = v_prefill.reshape(STRETCH, KVH, HD).astype(jnp.float32)

    def block(first_row):
        query_rows = lax.dynamic_slice_in_dim(q_prefill, first_row, TOK_DEV, 0)
        query_rows = query_rows.reshape(TOK_DEV, KVH, group_size, HD).astype(jnp.float32)
        query_pos = first_row + jnp.arange(TOK_DEV, dtype=jnp.int32)
        query_seg = lax.dynamic_slice_in_dim(all_seg, first_row, TOK_DEV, 0)
        scores = jnp.einsum('qkgd,nkd->kgqn', query_rows, keys_all) * score_scale
        visible = (query_seg[:, None] == all_seg[None, :]) & (all_pos[None, :] <= query_pos[:, None])
        scores = jnp.where(visible, scores, masked_score)
        row_max = lax.optimization_barrier(jnp.max(scores, axis=-1, keepdims=True))
        exp_terms = jnp.where(visible, jnp.exp(scores - row_max), 0.0)
        row_total = lax.optimization_barrier(jnp.sum(exp_terms, axis=-1))
        weights = exp_terms.astype(jnp.bfloat16).astype(jnp.float32)
        summed = jnp.einsum('kgqn,nkd->kgqd', weights, values_all) / row_total[..., None]
        return jnp.transpose(summed, (2, 0, 1, 3)).reshape(TOK_DEV, H * HD).astype(jnp.bfloat16)
    starts = jnp.arange(0, STRETCH, TOK_DEV, dtype=jnp.int32)
    attended = lax.map(block, starts).reshape(STRETCH, H * HD)
    dec_queries = q_decode.reshape(PROMPTS, KVH, group_size, HD).astype(jnp.float32)
    dec_keys = cache_k.reshape(PROMPTS, CACHE, KVH, HD).astype(jnp.float32)
    dec_values = cache_v.reshape(PROMPTS, CACHE, KVH, HD).astype(jnp.float32)
    dec_scores = jnp.einsum('pkgd,pckd->pkgc', dec_queries, dec_keys) * score_scale
    valid = (jnp.arange(CACHE, dtype=jnp.int32)[None, :] < cache_lengths[:, None])[:, None, None, :]
    dec_scores = jnp.where(valid, dec_scores, masked_score)
    dec_max = lax.optimization_barrier(jnp.max(dec_scores, axis=-1, keepdims=True))
    dec_exp = jnp.where(valid, jnp.exp(dec_scores - dec_max), 0.0)
    dec_total = lax.optimization_barrier(jnp.sum(dec_exp, axis=-1))
    dec_weights = dec_exp.astype(jnp.bfloat16).astype(jnp.float32)
    decode_out = jnp.einsum('pkgc,pckd->pkgd', dec_weights, dec_values) / dec_total[..., None]
    decode_out = decode_out.reshape(PROMPTS, H * HD).astype(jnp.bfloat16)
    verdict_in = jnp.concatenate([attended[pair_ends - 1], decode_out], axis=0)
    residual = stream.astype(jnp.float32) + jnp.dot(verdict_in, out_weight, preferred_element_type=jnp.float32)
    inv_rms = 1.0 / jnp.sqrt(lax.optimization_barrier(jnp.mean(residual * residual, axis=1)) + norm_eps)
    gained = residual * norm_gain.astype(jnp.float32)[None, :]
    verdict_hidden = (gained * inv_rms[:, None]).astype(jnp.bfloat16)
    table_rows = vocab_table[verdict_ids].astype(jnp.float32)
    verdict_logits = inv_rms[:, None] * lax.optimization_barrier(jnp.sum(gained[:, None, :] * table_rows, axis=2))
    win = 1.0 / (1.0 + jnp.exp(verdict_logits[:, 1] - verdict_logits[:, 0]))
    return (attended, verdict_hidden, win)
```

```python
import functools

import jax
import jax.numpy as jnp
from jax import lax
from jax.experimental import pallas as pl
from jax.experimental.pallas import tpu as pltpu
from jax.sharding import Mesh
from jax.sharding import PartitionSpec as P

D = 8192
H = 32
KVH = 8
HD = 128
PROMPTS = 4
PAIRS = 8
ROWS = 12
GROUP = H // KVH
LO = 8
SLOT = 16
KEY_BLOCK = 512
TP = ("tp_0", "tp_1")
SEQ = ("seq_hi", "seq_lo")

masked_score = -1e30
norm_eps = 1e-05
score_scale = 1.0 / HD**0.5
exp2_scale = score_scale * 1.4426950408889634

NT = (((1,), (1,)), ((), ()))
VM = pl.BlockSpec(memory_space=pltpu.VMEM)
SM = pl.BlockSpec(memory_space=pltpu.SMEM)


def exchanged(copies, axis):
    return lax.all_to_all(copies, axis, 0, 0, tiled=True)


def ends_of(lengths_ref):
    ends, total = [], 0
    for p in range(PAIRS):
        total = total + lengths_ref[p]
        ends.append(total)
    return ends


def last_rows_kernel(lengths_ref, seq_ref, q_ref, out_ref):
    tokens = q_ref.shape[0]
    ends = ends_of(lengths_ref)
    row = lax.broadcasted_iota(jnp.int32, (SLOT, tokens), 0)
    col = lax.broadcasted_iota(jnp.int32, (SLOT, tokens), 1) + seq_ref[0] * tokens
    last = jnp.full((SLOT, tokens), -1, jnp.int32)
    for p in range(PAIRS):
        last = jnp.where(row == p, ends[p] - 1, last)
    selector = jnp.where(col == last, 1.0, 0.0).astype(jnp.bfloat16)
    picked = jnp.dot(selector, q_ref[...], preferred_element_type=jnp.float32)
    for c in range(out_ref.shape[0]):
        out_ref[c] = picked[:PAIRS].astype(out_ref.dtype)


def partials_kernel(
    lengths_ref, cache_lengths_ref, seq_ref, rows_ref, qd_ref, k_ref, v_ref, ck_ref, cv_ref,
    out_ref, q_scratch,
):
    tokens = k_ref.shape[0]
    cache_count = ck_ref.shape[1]
    ends = ends_of(lengths_ref)
    q_scratch[...] = jnp.zeros_like(q_scratch)
    for g in range(GROUP):
        q_scratch[g * SLOT : g * SLOT + PAIRS, :] = rows_ref[:, g * HD : (g + 1) * HD]
        q_scratch[g * SLOT + PAIRS : g * SLOT + ROWS, :] = qd_ref[
            :, g * HD : (g + 1) * HD
        ].astype(jnp.float32)
    queries = q_scratch[...].astype(jnp.bfloat16)
    keys = jnp.concatenate([k_ref[...], ck_ref[...].reshape(PROMPTS * cache_count, HD)], axis=0)
    values = jnp.concatenate([v_ref[...], cv_ref[...].reshape(PROMPTS * cache_count, HD)], axis=0)
    count = tokens + PROMPTS * cache_count
    scores = lax.dot_general(queries, keys, NT, preferred_element_type=jnp.float32) * score_scale
    lane = lax.broadcasted_iota(jnp.int32, (1, count), 1)
    key_pos = lane + seq_ref[0] * tokens
    key_seg = jnp.zeros((1, count), jnp.int32)
    for p in range(PAIRS):
        key_seg = key_seg + jnp.where(key_pos >= ends[p], 1, 0)
    owner = key_seg
    for p in range(PROMPTS):
        first = tokens + p * cache_count
        mine = (lane >= first) & (lane < first + cache_count)
        cache_pos = lane - first + seq_ref[0] * cache_count
        label = jnp.where(cache_pos < cache_lengths_ref[p], PAIRS + p, -1)
        owner = jnp.where(mine, label, owner)
    item = lax.broadcasted_iota(jnp.int32, (GROUP * SLOT, count), 0) % SLOT
    visible = item == owner
    scores = jnp.where(visible, scores, masked_score)
    top = jnp.max(scores, axis=1, keepdims=True)
    terms = jnp.where(visible, jnp.exp(scores - top), 0.0)
    total = jnp.sum(terms, axis=1, keepdims=True)
    sums = jnp.dot(terms.astype(jnp.bfloat16), values, preferred_element_type=jnp.float32)
    put_partials(out_ref, sums, top, total)


def put_partials(out_ref, sums, top, total):
    across = (GROUP * SLOT, HD)
    top_lanes = jnp.transpose(jnp.broadcast_to(top, across))[:1]
    total_lanes = jnp.transpose(jnp.broadcast_to(total, across))[:1]
    for c in range(out_ref.shape[0]):
        out_ref[c] = sums
        out_ref[c, ROWS : ROWS + 1, : GROUP * SLOT] = top_lanes
        out_ref[c, ROWS + 1 : ROWS + 2, : GROUP * SLOT] = total_lanes


def merged(pieces_ref):
    count = pieces_ref.shape[0]
    tops, totals = [], []
    for c in range(count):
        both = pieces_ref[c, ROWS - 4 : ROWS + 4, :]
        columns = jnp.transpose(both)[: GROUP * SLOT]
        tops.append(columns[:, 4:5])
        totals.append(columns[:, 5:6])
    top = functools.reduce(jnp.maximum, tops)
    total = jnp.zeros_like(top)
    sums = jnp.zeros((GROUP * SLOT, HD), jnp.float32)
    for c in range(count):
        scale = jnp.exp(tops[c] - top)
        total = total + totals[c] * scale
        sums = sums + pieces_ref[c] * scale
    return sums, top, total


def merge_kernel(pieces_ref, out_ref):
    put_partials(out_ref, *merged(pieces_ref))


def project_kernel(pieces_ref, w_ref, table_ref, out_ref):
    sums, _, total = merged(pieces_ref)
    rows = sums / total
    partial = jnp.zeros((SLOT, w_ref.shape[1]), jnp.float32)
    for g in range(GROUP):
        partial = partial + jnp.dot(
            rows[g * SLOT : (g + 1) * SLOT].astype(jnp.bfloat16),
            w_ref[g * HD : (g + 1) * HD, :],
            preferred_element_type=jnp.float32,
        )
    keep = lax.broadcasted_iota(jnp.int32, partial.shape, 0) < ROWS
    partial = jnp.where(keep, partial, 0.0)
    for c in range(out_ref.shape[0]):
        out_ref[c, :SLOT] = partial
        out_ref[c, SLOT:] = table_ref[...]


def residual_kernel(pieces_ref, stream_ref, gain_ref, gained_ref, sums_ref):
    total = pieces_ref[0]
    for c in range(1, pieces_ref.shape[0]):
        total = total + pieces_ref[c]
    residual = total[:ROWS] + stream_ref[...].astype(jnp.float32)
    gained = residual * gain_ref[...].astype(jnp.float32)
    gained_ref[...] = gained
    squares = jnp.sum(residual * residual, axis=1, keepdims=True)
    first = jnp.sum(gained * total[SLOT : SLOT + ROWS], axis=1, keepdims=True)
    second = jnp.sum(gained * total[2 * SLOT : 2 * SLOT + ROWS], axis=1, keepdims=True)
    lane = lax.broadcasted_iota(jnp.int32, (ROWS, HD), 1)
    packed = jnp.where(lane == 0, squares, jnp.where(lane == 1, first, second))
    for c in range(sums_ref.shape[0]):
        sums_ref[c] = packed


def verdict_kernel(sums_ref, gained_ref, hidden_ref, win_ref):
    inv_rms = 1.0 / jnp.sqrt(sums_ref[:, 0:1] / D + norm_eps)
    hidden_ref[...] = (gained_ref[...] * inv_rms).astype(hidden_ref.dtype)
    logits = sums_ref[...] * inv_rms
    win = 1.0 / (1.0 + jnp.exp(logits[:, 2:3] - logits[:, 1:2]))
    win_ref[...] = jnp.broadcast_to(win, win_ref.shape)


def attention_kernel(
    lengths_ref, seq_ref, q_ref, kv_ref, out_ref, kv_buf, top_ref, total_ref, sum_ref, sems
):
    tokens = q_ref.shape[0]
    first = seq_ref[0] * tokens
    ends = ends_of(lengths_ref)
    start_first = jnp.int32(0)
    start_last = jnp.int32(0)
    for p in range(PAIRS):
        start_first = jnp.where(ends[p] <= first, ends[p], start_first)
        start_last = jnp.where(ends[p] <= first + tokens - 1, ends[p], start_last)
    low = start_first // KEY_BLOCK
    high = (first + tokens + KEY_BLOCK - 1) // KEY_BLOCK

    def fetch(b):
        rows = pl.ds(pl.multiple_of(b * KEY_BLOCK, KEY_BLOCK), KEY_BLOCK)
        return pltpu.make_async_copy(kv_ref.at[rows], kv_buf.at[rows], sems.at[b])

    def begin(b, carry):
        fetch(b).start()
        return carry

    lax.fori_loop(low, high, begin, 0)
    top_ref[...] = jnp.full_like(top_ref, masked_score)
    total_ref[...] = jnp.zeros_like(total_ref)
    sum_ref[...] = jnp.zeros_like(sum_ref)
    query_pos = lax.broadcasted_iota(jnp.int32, (tokens, 1), 0) + first
    query_start = jnp.zeros((tokens, 1), jnp.int32)
    for p in range(PAIRS):
        query_start = jnp.where(query_pos >= ends[p], ends[p], query_start)

    def attend(b, masked):
        key_first = b * KEY_BLOCK
        rows = pl.ds(pl.multiple_of(key_first, KEY_BLOCK), KEY_BLOCK)
        keys = kv_buf[rows, :HD]
        values = kv_buf[rows, HD:]
        if masked:
            key_pos = lax.broadcasted_iota(jnp.int32, (tokens, KEY_BLOCK), 1) + key_first
            visible = (key_pos >= query_start) & (key_pos <= query_pos)
        for g in range(GROUP):
            columns = slice(g * HD, (g + 1) * HD)
            scores = lax.dot_general(
                q_ref[:, columns], keys, NT, preferred_element_type=jnp.float32
            )
            if masked:
                scores = jnp.where(visible, scores, masked_score)
            old_top = top_ref[g]
            new_top = jnp.maximum(old_top, jnp.max(scores, axis=1, keepdims=True))
            rescale = jnp.exp2((old_top - new_top) * exp2_scale)
            terms = jnp.exp2((scores - new_top) * exp2_scale)
            lanes = terms[:, :HD]
            for j in range(1, KEY_BLOCK // HD):
                lanes = lanes + terms[:, j * HD : (j + 1) * HD]
            total_ref[g] = total_ref[g] * rescale + lanes
            sum_ref[g] = sum_ref[g] * rescale + jnp.dot(
                terms.astype(jnp.bfloat16), values, preferred_element_type=jnp.float32
            )
            top_ref[g] = new_top

    def step(b, carry):
        fetch(b).wait()
        key_first = b * KEY_BLOCK
        masked = (key_first < start_last) | (key_first + KEY_BLOCK > first + 1)

        @pl.when(masked)
        def _():
            attend(b, True)

        @pl.when(jnp.logical_not(masked))
        def _():
            attend(b, False)

        return carry

    lax.fori_loop(low, high, step, 0)
    for g in range(GROUP):
        total = jnp.sum(total_ref[g], axis=1, keepdims=True)
        out_ref[:, g * HD : (g + 1) * HD] = (sum_ref[g] / total).astype(out_ref.dtype)


def attention(lengths, seq_index, q, kv):
    tokens = q.shape[0]
    return pl.pallas_call(
        attention_kernel,
        out_shape=jax.ShapeDtypeStruct(q.shape, q.dtype),
        in_specs=[SM, SM, VM, pl.BlockSpec(memory_space=pl.ANY)],
        out_specs=VM,
        scratch_shapes=[
            pltpu.VMEM(kv.shape, kv.dtype),
            pltpu.VMEM((GROUP, tokens, 1), jnp.float32),
            pltpu.VMEM((GROUP, tokens, HD), jnp.float32),
            pltpu.VMEM((GROUP, tokens, HD), jnp.float32),
            pltpu.SemaphoreType.DMA((kv.shape[0] // KEY_BLOCK,)),
        ],
        compiler_params=pltpu.CompilerParams(vmem_limit_bytes=40 * 1024 * 1024),
        name="attention",
    )(lengths, seq_index, q, kv)


def call(kernel, shapes, specs, name, scratch=()):
    many = isinstance(shapes, tuple)
    return pl.pallas_call(
        kernel,
        out_shape=shapes,
        in_specs=specs,
        out_specs=tuple(VM for _ in shapes) if many else VM,
        scratch_shapes=list(scratch),
        name=name,
    )


def shards(
    q_prefill,
    k_prefill,
    v_prefill,
    pair_lengths,
    q_decode,
    cache_k,
    cache_v,
    cache_lengths,
    stream,
    out_weight,
    norm_gain,
    vocab_table,
    verdict_ids,
):
    f32 = jnp.float32
    lo = lax.axis_size("seq_lo")
    hi = lax.axis_size("seq_hi")
    tp = lax.axis_size(TP)
    columns = q_prefill.shape[1]
    width = stream.shape[1]
    seq_index = lax.axis_index(SEQ).astype(jnp.int32).reshape(1)
    shape = jax.ShapeDtypeStruct

    kv = lax.all_gather(jnp.concatenate([k_prefill, v_prefill], axis=1), SEQ, axis=0, tiled=True)

    picked = call(
        last_rows_kernel, shape((lo, PAIRS, columns), jnp.bfloat16), [SM, SM, VM], "last_rows"
    )(pair_lengths, seq_index, q_prefill)
    rows = jnp.sum(exchanged(picked, "seq_lo").astype(f32), axis=0)
    rows = lax.psum(rows, "seq_hi")

    partials = call(
        partials_kernel,
        shape((lo, GROUP * SLOT, HD), f32),
        [SM, SM, SM] + [VM] * 6,
        "partials",
        [pltpu.VMEM((GROUP * SLOT, HD), f32)],
    )(
        pair_lengths, cache_lengths, seq_index, rows, q_decode, k_prefill, v_prefill, cache_k,
        cache_v,
    )
    partials = exchanged(partials, "seq_lo")
    partials = call(merge_kernel, shape((hi, GROUP * SLOT, HD), f32), [VM], "merge")(partials)
    partials = exchanged(partials, "seq_hi")

    vocab_rows = vocab_table.shape[0]
    ids = jnp.pad(verdict_ids.T, ((0, 0), (0, SLOT - ROWS))).reshape(-1)
    local_ids = ids - lax.axis_index(TP) * vocab_rows
    inside = ((local_ids >= 0) & (local_ids < vocab_rows))[:, None]
    table_rows = vocab_table[jnp.clip(local_ids, 0, vocab_rows - 1)]
    table_rows = jnp.where(inside, table_rows.astype(f32), 0.0)

    pieces = call(
        project_kernel, shape((tp, 3 * SLOT, width), f32), [VM, VM, VM], "project"
    )(partials, out_weight, table_rows)
    pieces = exchanged(pieces, TP)
    gained, sums = call(
        residual_kernel,
        (shape((ROWS, width), f32), shape((lo, ROWS, HD), f32)),
        [VM, VM, VM],
        "residual",
    )(pieces, stream, norm_gain.reshape(1, width))
    sums = jnp.sum(exchanged(sums, "seq_lo"), axis=0)
    sums = lax.psum(sums, "seq_hi")
    verdict_hidden, win = call(
        verdict_kernel,
        (shape((ROWS, width), jnp.bfloat16), shape((ROWS, HD), f32)),
        [VM, VM],
        "verdict",
    )(sums, gained)

    attended = attention(pair_lengths, seq_index, q_prefill, kv)
    return (attended, verdict_hidden, win[:, 0])


def solution(mesh):
    groups, seq = mesh.shape["groups"], mesh.shape["seq"]
    torus = Mesh(
        mesh.devices.reshape(groups, seq // LO, LO, mesh.shape["tp"] // 2, 2),
        ("groups",) + SEQ + TP,
    )
    tokens = ("groups",) + SEQ
    return jax.shard_map(
        shards,
        mesh=torus,
        in_specs=(
            P(tokens, TP),
            P(tokens, TP),
            P(tokens, TP),
            P("groups"),
            P("groups", TP),
            P("groups", SEQ, TP),
            P("groups", SEQ, TP),
            P("groups"),
            P("groups", SEQ),
            P(TP, SEQ),
            P(SEQ),
            P(TP, SEQ),
            P("groups", None),
        ),
        out_specs=(P(tokens, TP), P("groups", SEQ), P("groups")),
        check_vma=False,
    )
```

```python
import functools

import jax
import jax.numpy as jnp
from jax import lax
from jax.experimental import pallas as pl
from jax.experimental.pallas import tpu as pltpu
from jax.sharding import Mesh
from jax.sharding import PartitionSpec as P

D = 8192
H = 32
KVH = 8
HD = 128
PROMPTS = 4
PAIRS = 8
ROWS = 12
GROUP = H // KVH
LO = 8
SLOT = 16
KEY_BLOCK = 512
TP = ("tp_0", "tp_1")
SEQ = ("seq_hi", "seq_lo")

masked_score = -1e30
norm_eps = 1e-05
score_scale = 1.0 / HD**0.5
exp2_scale = score_scale * 1.4426950408889634

NT = (((1,), (1,)), ((), ()))
VM = pl.BlockSpec(memory_space=pltpu.VMEM)
SM = pl.BlockSpec(memory_space=pltpu.SMEM)


def exchanged(copies, axis):
    return lax.all_to_all(copies, axis, 0, 0, tiled=True)


def ends_of(lengths_ref):
    ends, total = [], 0
    for p in range(PAIRS):
        total = total + lengths_ref[p]
        ends.append(total)
    return ends


def last_rows_kernel(lengths_ref, seq_ref, q_ref, k_ref, v_ref, out_ref, kv_ref):
    kv_ref[:, :HD] = k_ref[...]
    kv_ref[:, HD:] = v_ref[...]
    tokens = q_ref.shape[0]
    ends = ends_of(lengths_ref)
    row = lax.broadcasted_iota(jnp.int32, (SLOT, tokens), 0)
    col = lax.broadcasted_iota(jnp.int32, (SLOT, tokens), 1) + seq_ref[0] * tokens
    last = jnp.full((SLOT, tokens), -1, jnp.int32)
    for p in range(PAIRS):
        last = jnp.where(row == p, ends[p] - 1, last)
    selector = jnp.where(col == last, 1.0, 0.0).astype(jnp.bfloat16)
    picked = jnp.dot(selector, q_ref[...], preferred_element_type=jnp.float32)
    for c in range(out_ref.shape[0]):
        out_ref[c] = picked[:PAIRS].astype(out_ref.dtype)


def partials_kernel(
    lengths_ref, cache_lengths_ref, seq_ref, rows_ref, qd_ref, k_ref, v_ref, ck_ref, cv_ref,
    out_ref, q_scratch,
):
    tokens = k_ref.shape[0]
    cache_count = ck_ref.shape[1]
    ends = ends_of(lengths_ref)
    q_scratch[...] = jnp.zeros_like(q_scratch)
    for g in range(GROUP):
        q_scratch[g * SLOT : g * SLOT + PAIRS, :] = rows_ref[:, g * HD : (g + 1) * HD]
        q_scratch[g * SLOT + PAIRS : g * SLOT + ROWS, :] = qd_ref[
            :, g * HD : (g + 1) * HD
        ].astype(jnp.float32)
    queries = q_scratch[...].astype(jnp.bfloat16)
    keys = jnp.concatenate([k_ref[...], ck_ref[...].reshape(PROMPTS * cache_count, HD)], axis=0)
    values = jnp.concatenate([v_ref[...], cv_ref[...].reshape(PROMPTS * cache_count, HD)], axis=0)
    count = tokens + PROMPTS * cache_count
    scores = lax.dot_general(queries, keys, NT, preferred_element_type=jnp.float32) * score_scale
    lane = lax.broadcasted_iota(jnp.int32, (1, count), 1)
    key_pos = lane + seq_ref[0] * tokens
    key_seg = jnp.zeros((1, count), jnp.int32)
    for p in range(PAIRS):
        key_seg = key_seg + jnp.where(key_pos >= ends[p], 1, 0)
    owner = key_seg
    for p in range(PROMPTS):
        first = tokens + p * cache_count
        mine = (lane >= first) & (lane < first + cache_count)
        cache_pos = lane - first + seq_ref[0] * cache_count
        label = jnp.where(cache_pos < cache_lengths_ref[p], PAIRS + p, -1)
        owner = jnp.where(mine, label, owner)
    item = lax.broadcasted_iota(jnp.int32, (GROUP * SLOT, count), 0) % SLOT
    visible = item == owner
    scores = jnp.where(visible, scores, masked_score)
    top = jnp.max(scores, axis=1, keepdims=True)
    terms = jnp.where(visible, jnp.exp(scores - top), 0.0)
    total = jnp.sum(terms, axis=1, keepdims=True)
    sums = jnp.dot(terms.astype(jnp.bfloat16), values, preferred_element_type=jnp.float32)
    put_partials(out_ref, sums, top, total)


def three_parts(x):
    high = x.astype(jnp.bfloat16).astype(jnp.float32)
    middle = (x - high).astype(jnp.bfloat16).astype(jnp.float32)
    return high, middle, x - high - middle


def put_partials(out_ref, sums, top, total):
    across = (GROUP * SLOT, HD)
    row = lax.broadcasted_iota(jnp.int32, across, 0)
    packed = sums
    for first, column in ((ROWS, top), (SLOT + ROWS, total)):
        lanes = jnp.transpose(jnp.broadcast_to(column, across))[:1]
        lanes = jnp.concatenate([lanes, jnp.zeros_like(lanes)], axis=1)
        for j, part in enumerate(three_parts(lanes)):
            packed = jnp.where(row == first + j, part, packed)
    packed = packed.astype(out_ref.dtype)
    for c in range(out_ref.shape[0]):
        out_ref[c] = packed


def merged(pieces_ref):
    count = pieces_ref.shape[0]
    pieces = [pieces_ref[c].astype(jnp.float32) for c in range(count)]

    def columns(first):
        lines = [
            jnp.sum(piece[first : first + 3], axis=0, keepdims=True) for piece in pieces
        ] + [jnp.zeros((8 - count % 8, HD), jnp.float32)] * (count % 8 > 0)
        turned = jnp.transpose(jnp.concatenate(lines, axis=0))[: GROUP * SLOT]
        return [turned[:, c : c + 1] for c in range(count)]

    tops, totals = columns(ROWS), columns(SLOT + ROWS)
    top = functools.reduce(jnp.maximum, tops)
    total = jnp.zeros_like(top)
    sums = jnp.zeros((GROUP * SLOT, HD), jnp.float32)
    for c in range(count):
        scale = jnp.exp(tops[c] - top)
        total = total + totals[c] * scale
        sums = sums + pieces[c] * scale
    return sums, top, total


def merge_kernel(pieces_ref, out_ref):
    put_partials(out_ref, *merged(pieces_ref))


def project_kernel(pieces_ref, w_ref, table_ref, out_ref):
    sums, _, total = merged(pieces_ref)
    rows = sums / total
    partial = jnp.zeros((SLOT, w_ref.shape[1]), jnp.float32)
    for g in range(GROUP):
        partial = partial + jnp.dot(
            rows[g * SLOT : (g + 1) * SLOT].astype(jnp.bfloat16),
            w_ref[g * HD : (g + 1) * HD, :],
            preferred_element_type=jnp.float32,
        )
    for c in range(out_ref.shape[0]):
        out_ref[c, :ROWS] = partial[:ROWS]
        out_ref[c, ROWS : 3 * ROWS] = table_ref[...]


def residual_kernel(pieces_ref, stream_ref, gain_ref, gained_ref, sums_ref):
    total = pieces_ref[0]
    for c in range(1, pieces_ref.shape[0]):
        total = total + pieces_ref[c]
    residual = total[:ROWS] + stream_ref[...].astype(jnp.float32)
    gained = residual * gain_ref[...].astype(jnp.float32)
    gained_ref[...] = gained
    squares = jnp.sum(residual * residual, axis=1, keepdims=True)
    first = jnp.sum(gained * total[ROWS : 2 * ROWS], axis=1, keepdims=True)
    second = jnp.sum(gained * total[2 * ROWS : 3 * ROWS], axis=1, keepdims=True)
    lane = lax.broadcasted_iota(jnp.int32, (ROWS, HD), 1)
    packed = jnp.where(lane == 0, squares, jnp.where(lane == 1, first, second))
    for c in range(sums_ref.shape[0]):
        sums_ref[c] = packed


def verdict_kernel(sums_ref, gained_ref, hidden_ref, win_ref):
    inv_rms = 1.0 / jnp.sqrt(sums_ref[:, 0:1] / D + norm_eps)
    hidden_ref[...] = (gained_ref[...] * inv_rms).astype(hidden_ref.dtype)
    logits = sums_ref[...] * inv_rms
    win = 1.0 / (1.0 + jnp.exp(logits[:, 2:3] - logits[:, 1:2]))
    win_ref[...] = jnp.broadcast_to(win, win_ref.shape)


def attention_kernel(
    lengths_ref, seq_ref, q_ref, kv_ref, out_ref, kv_buf, top_ref, total_ref, sum_ref, sems
):
    tokens = q_ref.shape[0]
    first = seq_ref[0] * tokens
    ends = ends_of(lengths_ref)
    start_first = jnp.int32(0)
    start_last = jnp.int32(0)
    for p in range(PAIRS):
        start_first = jnp.where(ends[p] <= first, ends[p], start_first)
        start_last = jnp.where(ends[p] <= first + tokens - 1, ends[p], start_last)
    low = start_first // KEY_BLOCK
    high = (first + tokens + KEY_BLOCK - 1) // KEY_BLOCK

    def fetch(b):
        rows = pl.ds(pl.multiple_of(b * KEY_BLOCK, KEY_BLOCK), KEY_BLOCK)
        return pltpu.make_async_copy(kv_ref.at[rows], kv_buf.at[rows], sems.at[b])

    def begin(b, carry):
        fetch(b).start()
        return carry

    lax.fori_loop(low, high, begin, 0)
    top_ref[...] = jnp.full_like(top_ref, masked_score)
    total_ref[...] = jnp.zeros_like(total_ref)
    sum_ref[...] = jnp.zeros_like(sum_ref)
    query_pos = lax.broadcasted_iota(jnp.int32, (1, tokens), 1) + first
    query_start = jnp.zeros((1, tokens), jnp.int32)
    for p in range(PAIRS):
        query_start = jnp.where(query_pos >= ends[p], ends[p], query_start)

    def attend(b, masked):
        key_first = b * KEY_BLOCK
        rows = pl.ds(pl.multiple_of(key_first, KEY_BLOCK), KEY_BLOCK)
        keys = kv_buf[rows, :HD]
        values = jnp.transpose(kv_buf[rows, HD:])
        if masked:
            key_pos = lax.broadcasted_iota(jnp.int32, (KEY_BLOCK, tokens), 0) + key_first
            visible = (key_pos >= query_start) & (key_pos <= query_pos)
        for g in range(GROUP):
            queries = q_ref[:, g * HD : (g + 1) * HD]
            scores = lax.dot_general(keys, queries, NT, preferred_element_type=jnp.float32)
            if masked:
                scores = jnp.where(visible, scores, masked_score)
            old_top = top_ref[g]
            tops = jnp.max(scores.reshape(KEY_BLOCK // 8, 8, tokens), axis=0)
            new_top = jnp.maximum(old_top, jnp.max(tops, axis=0, keepdims=True))
            rescale = jnp.exp2((old_top - new_top) * exp2_scale)
            terms = jnp.exp2((scores - new_top) * exp2_scale)
            sums = jnp.sum(terms.reshape(KEY_BLOCK // 8, 8, tokens), axis=0)
            total_ref[g] = total_ref[g] * rescale + sums
            sum_ref[g] = sum_ref[g] * rescale + jnp.dot(
                values, terms.astype(jnp.bfloat16), preferred_element_type=jnp.float32
            )
            top_ref[g] = new_top

    def step(b, carry):
        fetch(b).wait()
        key_first = b * KEY_BLOCK
        masked = (key_first < start_last) | (key_first + KEY_BLOCK > first + 1)

        @pl.when(masked)
        def _():
            attend(b, True)

        @pl.when(jnp.logical_not(masked))
        def _():
            attend(b, False)

        return carry

    lax.fori_loop(low, high, step, 0)
    for g in range(GROUP):
        total = jnp.sum(total_ref[g], axis=0, keepdims=True)
        rows = jnp.transpose(sum_ref[g] / total)
        out_ref[:, g * HD : (g + 1) * HD] = rows.astype(out_ref.dtype)


def attention(lengths, seq_index, q, kv):
    tokens = q.shape[0]
    return pl.pallas_call(
        attention_kernel,
        out_shape=jax.ShapeDtypeStruct(q.shape, q.dtype),
        in_specs=[SM, SM, VM, pl.BlockSpec(memory_space=pltpu.HBM)],
        out_specs=VM,
        scratch_shapes=[
            pltpu.VMEM(kv.shape, kv.dtype),
            pltpu.VMEM((GROUP, 1, tokens), jnp.float32),
            pltpu.VMEM((GROUP, 8, tokens), jnp.float32),
            pltpu.VMEM((GROUP, HD, tokens), jnp.float32),
            pltpu.SemaphoreType.DMA((kv.shape[0] // KEY_BLOCK,)),
        ],
        compiler_params=pltpu.CompilerParams(vmem_limit_bytes=24 * 1024 * 1024),
        name="attention",
    )(lengths, seq_index, q, kv)


def call(kernel, shapes, specs, name, scratch=()):
    many = isinstance(shapes, tuple)
    return pl.pallas_call(
        kernel,
        out_shape=shapes,
        in_specs=specs,
        out_specs=tuple(VM for _ in shapes) if many else VM,
        scratch_shapes=list(scratch),
        compiler_params=pltpu.CompilerParams(vmem_limit_bytes=8 * 1024 * 1024),
        name=name,
    )


def shards(
    q_prefill,
    k_prefill,
    v_prefill,
    pair_lengths,
    q_decode,
    cache_k,
    cache_v,
    cache_lengths,
    stream,
    out_weight,
    norm_gain,
    vocab_table,
    verdict_ids,
):
    f32 = jnp.float32
    lo = lax.axis_size("seq_lo")
    hi = lax.axis_size("seq_hi")
    tp = lax.axis_size(TP)
    columns = q_prefill.shape[1]
    width = stream.shape[1]
    seq_index = lax.axis_index(SEQ).astype(jnp.int32).reshape(1)
    shape = jax.ShapeDtypeStruct

    picked, kv = call(
        last_rows_kernel,
        (
            shape((lo, PAIRS, columns), jnp.bfloat16),
            shape((q_prefill.shape[0], 2 * HD), jnp.bfloat16),
        ),
        [SM, SM, VM, VM, VM],
        "last_rows",
    )(pair_lengths, seq_index, q_prefill, k_prefill, v_prefill)
    kv = lax.all_gather(kv, SEQ, axis=0, tiled=True)
    rows = jnp.sum(exchanged(picked, "seq_lo").astype(f32), axis=0)
    rows = lax.psum(rows, "seq_hi")

    partials = call(
        partials_kernel,
        shape((lo, GROUP * SLOT, HD), jnp.bfloat16),
        [SM, SM, SM] + [VM] * 6,
        "partials",
        [pltpu.VMEM((GROUP * SLOT, HD), f32)],
    )(
        pair_lengths, cache_lengths, seq_index, rows, q_decode, k_prefill, v_prefill, cache_k,
        cache_v,
    )
    partials = exchanged(partials, "seq_lo")
    partials = call(merge_kernel, shape((hi, GROUP * SLOT, HD), jnp.bfloat16), [VM], "merge")(partials)
    partials = exchanged(partials, "seq_hi")

    vocab_rows = vocab_table.shape[0]
    ids = verdict_ids.T.reshape(-1)
    local_ids = ids - lax.axis_index(TP) * vocab_rows
    inside = ((local_ids >= 0) & (local_ids < vocab_rows))[:, None]
    table_rows = vocab_table[jnp.clip(local_ids, 0, vocab_rows - 1)]
    table_rows = jnp.where(inside, table_rows.astype(f32), 0.0)

    pieces = call(
        project_kernel, shape((tp, 3 * ROWS, width), f32), [VM, VM, VM], "project"
    )(partials, out_weight, table_rows)
    pieces = exchanged(pieces, TP)
    gained, sums = call(
        residual_kernel,
        (shape((ROWS, width), f32), shape((lo, ROWS, HD), f32)),
        [VM, VM, VM],
        "residual",
    )(pieces, stream, norm_gain.reshape(1, width))
    sums = jnp.sum(exchanged(sums, "seq_lo"), axis=0)
    sums = lax.psum(sums, "seq_hi")
    verdict_hidden, win = call(
        verdict_kernel,
        (shape((ROWS, width), jnp.bfloat16), shape((ROWS, HD), f32)),
        [VM, VM],
        "verdict",
    )(sums, gained)

    attended = attention(pair_lengths, seq_index, q_prefill, kv)
    return (attended, verdict_hidden, win[:, 0])


def solution(mesh):
    groups, seq = mesh.shape["groups"], mesh.shape["seq"]
    torus = Mesh(
        mesh.devices.reshape(groups, seq // LO, LO, mesh.shape["tp"] // 2, 2),
        ("groups",) + SEQ + TP,
    )
    tokens = ("groups",) + SEQ
    return jax.shard_map(
        shards,
        mesh=torus,
        in_specs=(
            P(tokens, TP),
            P(tokens, TP),
            P(tokens, TP),
            P("groups"),
            P("groups", TP),
            P("groups", SEQ, TP),
            P("groups", SEQ, TP),
            P("groups"),
            P("groups", SEQ),
            P(TP, SEQ),
            P(SEQ),
            P(TP, SEQ),
            P("groups", None),
        ),
        out_specs=(P(tokens, TP), P("groups", SEQ), P("groups")),
        check_vma=False,
    )
```

```python
import functools

import jax
import jax.numpy as jnp
from jax import lax
from jax.experimental import pallas as pl
from jax.experimental.pallas import tpu as pltpu
from jax.sharding import Mesh
from jax.sharding import PartitionSpec as P

D = 8192
H = 32
KVH = 8
HD = 128
PROMPTS = 4
PAIRS = 8
ROWS = 12
GROUP = H // KVH
LO = 8
SLOT = 16
KEY_BLOCK = 512
TP = ("tp_0", "tp_1")
SEQ = ("seq_hi", "seq_lo")

masked_score = -1e30
norm_eps = 1e-05
score_scale = 1.0 / HD**0.5
exp2_scale = score_scale * 1.4426950408889634

NT = (((1,), (1,)), ((), ()))
VM = pl.BlockSpec(memory_space=pltpu.VMEM)
SM = pl.BlockSpec(memory_space=pltpu.SMEM)
HB = pl.BlockSpec(memory_space=pltpu.HBM)
PIPE = pl.BlockSpec()
TABLE_ROWS = 16


def held(x):
    return pltpu.with_memory_space_constraint(x, pltpu.HBM)


def exchanged(copies, axis):
    return lax.all_to_all(copies, axis, 0, 0, tiled=True)


def ends_of(lengths_ref):
    ends, total = [], 0
    for p in range(PAIRS):
        total = total + lengths_ref[p]
        ends.append(total)
    return ends


def last_rows_kernel(lengths_ref, seq_ref, q_ref, k_ref, v_ref, out_ref, kv_ref):
    kv_ref[:, :HD] = k_ref[...]
    kv_ref[:, HD:] = v_ref[...]
    tokens = q_ref.shape[0]
    ends = ends_of(lengths_ref)
    row = lax.broadcasted_iota(jnp.int32, (SLOT, tokens), 0)
    col = lax.broadcasted_iota(jnp.int32, (SLOT, tokens), 1) + seq_ref[0] * tokens
    last = jnp.full((SLOT, tokens), -1, jnp.int32)
    for p in range(PAIRS):
        last = jnp.where(row == p, ends[p] - 1, last)
    selector = jnp.where(col == last, 1.0, 0.0).astype(jnp.bfloat16)
    picked = jnp.dot(selector, q_ref[...], preferred_element_type=jnp.float32)
    for c in range(out_ref.shape[0]):
        out_ref[c] = picked[:PAIRS].astype(out_ref.dtype)


def partials_kernel(
    lengths_ref, cache_lengths_ref, seq_ref, rows_ref, qd_ref, k_ref, v_ref, ck_ref, cv_ref,
    out_ref, q_scratch,
):
    tokens = k_ref.shape[0]
    cache_count = ck_ref.shape[1]
    ends = ends_of(lengths_ref)
    q_scratch[...] = jnp.zeros_like(q_scratch)
    for g in range(GROUP):
        q_scratch[g * SLOT : g * SLOT + PAIRS, :] = rows_ref[
            :, g * HD : (g + 1) * HD
        ].astype(jnp.float32)
        q_scratch[g * SLOT + PAIRS : g * SLOT + ROWS, :] = qd_ref[
            :, g * HD : (g + 1) * HD
        ].astype(jnp.float32)
    queries = q_scratch[...].astype(jnp.bfloat16)
    keys = jnp.concatenate([k_ref[...], ck_ref[...].reshape(PROMPTS * cache_count, HD)], axis=0)
    values = jnp.concatenate([v_ref[...], cv_ref[...].reshape(PROMPTS * cache_count, HD)], axis=0)
    count = tokens + PROMPTS * cache_count
    scores = lax.dot_general(queries, keys, NT, preferred_element_type=jnp.float32) * score_scale
    lane = lax.broadcasted_iota(jnp.int32, (1, count), 1)
    key_pos = lane + seq_ref[0] * tokens
    key_seg = jnp.zeros((1, count), jnp.int32)
    for p in range(PAIRS):
        key_seg = key_seg + jnp.where(key_pos >= ends[p], 1, 0)
    owner = key_seg
    for p in range(PROMPTS):
        first = tokens + p * cache_count
        mine = (lane >= first) & (lane < first + cache_count)
        cache_pos = lane - first + seq_ref[0] * cache_count
        label = jnp.where(cache_pos < cache_lengths_ref[p], PAIRS + p, -1)
        owner = jnp.where(mine, label, owner)
    item = lax.broadcasted_iota(jnp.int32, (GROUP * SLOT, count), 0) % SLOT
    visible = item == owner
    scores = jnp.where(visible, scores, masked_score)
    top = jnp.max(scores, axis=1, keepdims=True)
    terms = jnp.where(visible, jnp.exp(scores - top), 0.0)
    total = jnp.sum(terms, axis=1, keepdims=True)
    sums = jnp.dot(terms.astype(jnp.bfloat16), values, preferred_element_type=jnp.float32)
    put_partials(out_ref, sums, top, total)


def three_parts(x):
    high = x.astype(jnp.bfloat16).astype(jnp.float32)
    middle = (x - high).astype(jnp.bfloat16).astype(jnp.float32)
    return high, middle, x - high - middle


def put_partials(out_ref, sums, top, total):
    across = (GROUP * SLOT, HD)
    row = lax.broadcasted_iota(jnp.int32, across, 0)
    packed = sums
    for first, column in ((ROWS, top), (SLOT + ROWS, total)):
        lanes = jnp.transpose(jnp.broadcast_to(column, across))[:1]
        lanes = jnp.concatenate([lanes, jnp.zeros_like(lanes)], axis=1)
        for j, part in enumerate(three_parts(lanes)):
            packed = jnp.where(row == first + j, part, packed)
    packed = packed.astype(out_ref.dtype)
    for c in range(out_ref.shape[0]):
        out_ref[c] = packed


def merged(pieces_ref):
    count = pieces_ref.shape[0]
    pieces = [pieces_ref[c].astype(jnp.float32) for c in range(count)]

    def columns(first):
        lines = [
            jnp.sum(piece[first : first + 3], axis=0, keepdims=True) for piece in pieces
        ] + [jnp.zeros((8 - count % 8, HD), jnp.float32)] * (count % 8 > 0)
        turned = jnp.transpose(jnp.concatenate(lines, axis=0))[: GROUP * SLOT]
        return [turned[:, c : c + 1] for c in range(count)]

    tops, totals = columns(ROWS), columns(SLOT + ROWS)
    top = functools.reduce(jnp.maximum, tops)
    total = jnp.zeros_like(top)
    sums = jnp.zeros((GROUP * SLOT, HD), jnp.float32)
    for c in range(count):
        scale = jnp.exp(tops[c] - top)
        total = total + totals[c] * scale
        sums = sums + pieces[c] * scale
    return sums, top, total


def merge_kernel(pieces_ref, out_ref):
    put_partials(out_ref, *merged(pieces_ref))


def project_kernel(
    ids_ref, tp_ref, pieces_ref, w_ref, table_ref, out_ref, blocks, rows_scratch, sems
):
    vocab_rows = table_ref.shape[0]
    picks = []
    for c in range(2):
        for r in range(ROWS):
            local = ids_ref[r, c] - tp_ref[0] * vocab_rows
            inside = (local >= 0) & (local < vocab_rows)
            local = jnp.clip(local, 0, vocab_rows - 1)
            picks.append((jnp.where(inside, local % TABLE_ROWS, -1), local // TABLE_ROWS))
    copies = []
    for i, (_, block) in enumerate(picks):
        rows = pl.ds(pl.multiple_of(block * TABLE_ROWS, TABLE_ROWS), TABLE_ROWS)
        copies.append(pltpu.make_async_copy(table_ref.at[rows], blocks.at[i], sems.at[i]))
        copies[-1].start()
    sums, _, total = merged(pieces_ref)
    rows = sums / total
    partial = jnp.zeros((SLOT, w_ref.shape[1]), jnp.float32)
    for g in range(GROUP):
        partial = partial + jnp.dot(
            rows[g * SLOT : (g + 1) * SLOT].astype(jnp.bfloat16),
            w_ref[g * HD : (g + 1) * HD, :],
            preferred_element_type=jnp.float32,
        )
    for copy in copies:
        copy.wait()
    index = lax.broadcasted_iota(jnp.int32, (TABLE_ROWS, w_ref.shape[1]), 0)
    for i, (row, _) in enumerate(picks):
        block = jnp.where(index == row, blocks[i].astype(jnp.float32), 0.0)
        rows_scratch[i : i + 1, :] = jnp.sum(block, axis=0, keepdims=True)
    for c in range(out_ref.shape[0]):
        out_ref[c, :ROWS] = partial[:ROWS]
        out_ref[c, ROWS : 3 * ROWS] = rows_scratch[...]


def residual_kernel(pieces_ref, stream_ref, gain_ref, gained_ref, sums_ref):
    total = pieces_ref[0]
    for c in range(1, pieces_ref.shape[0]):
        total = total + pieces_ref[c]
    residual = total[:ROWS] + stream_ref[...].astype(jnp.float32)
    gained = residual * gain_ref[...].astype(jnp.float32)
    gained_ref[...] = gained
    squares = jnp.sum(residual * residual, axis=1, keepdims=True)
    first = jnp.sum(gained * total[ROWS : 2 * ROWS], axis=1, keepdims=True)
    second = jnp.sum(gained * total[2 * ROWS : 3 * ROWS], axis=1, keepdims=True)
    lane = lax.broadcasted_iota(jnp.int32, (ROWS, HD), 1)
    packed = jnp.where(lane == 0, squares, jnp.where(lane == 1, first, second))
    for c in range(sums_ref.shape[0]):
        sums_ref[c] = packed


def verdict_kernel(sums_ref, gained_ref, hidden_ref, win_ref):
    inv_rms = 1.0 / jnp.sqrt(sums_ref[:, 0:1] / D + norm_eps)
    hidden_ref[...] = (gained_ref[...] * inv_rms).astype(hidden_ref.dtype)
    logits = sums_ref[...] * inv_rms
    win = 1.0 / (1.0 + jnp.exp(logits[:, 2:3] - logits[:, 1:2]))
    win_ref[...] = jnp.broadcast_to(win, win_ref.shape)


def attention_kernel(
    lengths_ref, seq_ref, q_ref, kv_ref, out_ref, kv_buf, top_ref, total_ref, sum_ref, sems
):
    tokens = q_ref.shape[0]
    first = seq_ref[0] * tokens
    ends = ends_of(lengths_ref)
    start_first = jnp.int32(0)
    start_last = jnp.int32(0)
    for p in range(PAIRS):
        start_first = jnp.where(ends[p] <= first, ends[p], start_first)
        start_last = jnp.where(ends[p] <= first + tokens - 1, ends[p], start_last)
    low = start_first // KEY_BLOCK
    high = (first + tokens + KEY_BLOCK - 1) // KEY_BLOCK

    def fetch(b):
        rows = pl.ds(pl.multiple_of(b * KEY_BLOCK, KEY_BLOCK), KEY_BLOCK)
        return pltpu.make_async_copy(kv_ref.at[rows], kv_buf.at[rows], sems.at[b])

    def begin(b, carry):
        fetch(b).start()
        return carry

    lax.fori_loop(low, high, begin, 0)
    top_ref[...] = jnp.full_like(top_ref, masked_score)
    total_ref[...] = jnp.zeros_like(total_ref)
    sum_ref[...] = jnp.zeros_like(sum_ref)
    query_pos = lax.broadcasted_iota(jnp.int32, (1, tokens), 1) + first
    query_start = jnp.zeros((1, tokens), jnp.int32)
    for p in range(PAIRS):
        query_start = jnp.where(query_pos >= ends[p], ends[p], query_start)

    def attend(b, masked):
        key_first = b * KEY_BLOCK
        rows = pl.ds(pl.multiple_of(key_first, KEY_BLOCK), KEY_BLOCK)
        keys = kv_buf[rows, :HD]
        values = jnp.transpose(kv_buf[rows, HD:])
        if masked:
            key_pos = lax.broadcasted_iota(jnp.int32, (KEY_BLOCK, tokens), 0) + key_first
            visible = (key_pos >= query_start) & (key_pos <= query_pos)
        for g in range(GROUP):
            queries = q_ref[:, g * HD : (g + 1) * HD]
            scores = lax.dot_general(keys, queries, NT, preferred_element_type=jnp.float32)
            if masked:
                scores = jnp.where(visible, scores, masked_score)
            old_top = top_ref[g]
            tops = jnp.max(scores.reshape(KEY_BLOCK // 8, 8, tokens), axis=0)
            new_top = jnp.maximum(old_top, jnp.max(tops, axis=0, keepdims=True))
            rescale = jnp.exp2((old_top - new_top) * exp2_scale)
            terms = jnp.exp2((scores - new_top) * exp2_scale)
            sums = jnp.sum(terms.reshape(KEY_BLOCK // 8, 8, tokens), axis=0)
            total_ref[g] = total_ref[g] * rescale + sums
            sum_ref[g] = sum_ref[g] * rescale + jnp.dot(
                values, terms.astype(jnp.bfloat16), preferred_element_type=jnp.float32
            )
            top_ref[g] = new_top

    def step(b, carry):
        fetch(b).wait()
        key_first = b * KEY_BLOCK
        masked = (key_first < start_last) | (key_first + KEY_BLOCK > first + 1)

        @pl.when(masked)
        def _():
            attend(b, True)

        @pl.when(jnp.logical_not(masked))
        def _():
            attend(b, False)

        return carry

    lax.fori_loop(low, high, step, 0)
    for g in range(GROUP):
        total = jnp.sum(total_ref[g], axis=0, keepdims=True)
        rows = jnp.transpose(sum_ref[g] / total)
        out_ref[:, g * HD : (g + 1) * HD] = rows.astype(out_ref.dtype)


def attention(lengths, seq_index, q, kv):
    tokens = q.shape[0]
    return pl.pallas_call(
        attention_kernel,
        out_shape=jax.ShapeDtypeStruct(q.shape, q.dtype),
        in_specs=[SM, SM, PIPE, HB],
        out_specs=VM,
        scratch_shapes=[
            pltpu.VMEM(kv.shape, kv.dtype),
            pltpu.VMEM((GROUP, 1, tokens), jnp.float32),
            pltpu.VMEM((GROUP, 8, tokens), jnp.float32),
            pltpu.VMEM((GROUP, HD, tokens), jnp.float32),
            pltpu.SemaphoreType.DMA((kv.shape[0] // KEY_BLOCK,)),
        ],
        compiler_params=pltpu.CompilerParams(vmem_limit_bytes=24 * 1024 * 1024),
        name="attention",
    )(lengths, seq_index, held(q), held(kv))


def call(kernel, shapes, specs, name, scratch=()):
    many = isinstance(shapes, tuple)
    return pl.pallas_call(
        kernel,
        out_shape=shapes,
        in_specs=specs,
        out_specs=tuple(VM for _ in shapes) if many else VM,
        scratch_shapes=list(scratch),
        compiler_params=pltpu.CompilerParams(vmem_limit_bytes=8 * 1024 * 1024),
        name=name,
    )


def shards(
    q_prefill,
    k_prefill,
    v_prefill,
    pair_lengths,
    q_decode,
    cache_k,
    cache_v,
    cache_lengths,
    stream,
    out_weight,
    norm_gain,
    vocab_table,
    verdict_ids,
):
    f32 = jnp.float32
    lo = lax.axis_size("seq_lo")
    hi = lax.axis_size("seq_hi")
    tp = lax.axis_size(TP)
    columns = q_prefill.shape[1]
    width = stream.shape[1]
    pair_lengths, cache_lengths = held(pair_lengths), held(cache_lengths)
    seq_index = lax.axis_index(SEQ).astype(jnp.int32).reshape(1)
    shape = jax.ShapeDtypeStruct

    picked, kv = call(
        last_rows_kernel,
        (
            shape((lo, PAIRS, columns), jnp.bfloat16),
            shape((q_prefill.shape[0], 2 * HD), jnp.bfloat16),
        ),
        [SM, SM, PIPE, PIPE, PIPE],
        "last_rows",
    )(pair_lengths, seq_index, held(q_prefill), held(k_prefill), held(v_prefill))
    kv = lax.all_gather(kv, SEQ, axis=0, tiled=True)
    rows = jnp.sum(exchanged(picked, "seq_lo").astype(f32), axis=0)
    rows = lax.psum(rows.astype(jnp.bfloat16), "seq_hi")

    partials = call(
        partials_kernel,
        shape((lo, GROUP * SLOT, HD), jnp.bfloat16),
        [SM, SM, SM, VM] + [PIPE] * 5,
        "partials",
        [pltpu.VMEM((GROUP * SLOT, HD), f32)],
    )(
        pair_lengths, cache_lengths, seq_index, rows, held(q_decode), held(k_prefill),
        held(v_prefill), held(cache_k), held(cache_v),
    )
    partials = exchanged(partials, "seq_lo")
    partials = call(merge_kernel, shape((hi, GROUP * SLOT, HD), jnp.bfloat16), [VM], "merge")(partials)
    partials = exchanged(partials, "seq_hi")

    tp_index = lax.axis_index(TP).astype(jnp.int32).reshape(1)
    pieces = call(
        project_kernel,
        shape((tp, 3 * ROWS, width), f32),
        [SM, SM, VM, PIPE, HB],
        "project",
        [
            pltpu.VMEM((2 * ROWS, TABLE_ROWS, width), jnp.bfloat16),
            pltpu.VMEM((2 * ROWS, width), f32),
            pltpu.SemaphoreType.DMA((2 * ROWS,)),
        ],
    )(verdict_ids, tp_index, partials, held(out_weight), held(vocab_table))
    pieces = exchanged(pieces, TP)
    gained, sums = call(
        residual_kernel,
        (shape((ROWS, width), f32), shape((lo, ROWS, HD), f32)),
        [VM, PIPE, PIPE],
        "residual",
    )(pieces, held(stream), held(norm_gain.reshape(1, width)))
    sums = jnp.sum(exchanged(sums, "seq_lo"), axis=0)
    sums = lax.psum(sums, "seq_hi")
    verdict_hidden, win = call(
        verdict_kernel,
        (shape((ROWS, width), jnp.bfloat16), shape((ROWS, HD), f32)),
        [VM, VM],
        "verdict",
    )(sums, gained)

    attended = attention(pair_lengths, seq_index, q_prefill, kv)
    return (attended, verdict_hidden, win[:, 0])


def solution(mesh):
    groups, seq = mesh.shape["groups"], mesh.shape["seq"]
    torus = Mesh(
        mesh.devices.reshape(groups, seq // LO, LO, mesh.shape["tp"] // 2, 2),
        ("groups",) + SEQ + TP,
    )
    tokens = ("groups",) + SEQ
    return jax.shard_map(
        shards,
        mesh=torus,
        in_specs=(
            P(tokens, TP),
            P(tokens, TP),
            P(tokens, TP),
            P("groups"),
            P("groups", TP),
            P("groups", SEQ, TP),
            P("groups", SEQ, TP),
            P("groups"),
            P("groups", SEQ),
            P(TP, SEQ),
            P(SEQ),
            P(TP, SEQ),
            P("groups", None),
        ),
        out_specs=(P(tokens, TP), P("groups", SEQ), P("groups")),
        check_vma=False,
    )
```

```python
import functools

import jax
import jax.numpy as jnp
from jax import lax
from jax.experimental import pallas as pl
from jax.experimental.pallas import tpu as pltpu
from jax.sharding import Mesh
from jax.sharding import PartitionSpec as P

D = 8192
H = 32
KVH = 8
HD = 128
PROMPTS = 4
PAIRS = 8
ROWS = 12
GROUP = H // KVH
LO = 8
SLOT = 16
KEY_BLOCK = 256
TP = ("tp_0", "tp_1")
SEQ = ("seq_hi", "seq_lo")

masked_score = -1e30
norm_eps = 1e-05
score_scale = 1.0 / HD**0.5
exp2_scale = score_scale * 1.4426950408889634

NT = (((1,), (1,)), ((), ()))
VM = pl.BlockSpec(memory_space=pltpu.VMEM)
SM = pl.BlockSpec(memory_space=pltpu.SMEM)
HB = pl.BlockSpec(memory_space=pltpu.HBM)
PIPE = pl.BlockSpec()
TABLE_ROWS = 16


def held(x):
    return pltpu.with_memory_space_constraint(x, pltpu.HBM)


def exchanged(copies, axis):
    return lax.all_to_all(copies, axis, 0, 0, tiled=True)


def ends_of(lengths_ref):
    ends, total = [], 0
    for p in range(PAIRS):
        total = total + lengths_ref[p]
        ends.append(total)
    return ends


def last_rows_kernel(lengths_ref, seq_ref, q_ref, k_ref, v_ref, out_ref, kv_ref):
    kv_ref[:, :HD] = k_ref[...]
    kv_ref[:, HD:] = v_ref[...]
    tokens = q_ref.shape[0]
    ends = ends_of(lengths_ref)
    row = lax.broadcasted_iota(jnp.int32, (SLOT, tokens), 0)
    col = lax.broadcasted_iota(jnp.int32, (SLOT, tokens), 1) + seq_ref[0] * tokens
    last = jnp.full((SLOT, tokens), -1, jnp.int32)
    for p in range(PAIRS):
        last = jnp.where(row == p, ends[p] - 1, last)
    selector = jnp.where(col == last, 1.0, 0.0).astype(jnp.bfloat16)
    picked = jnp.dot(selector, q_ref[...], preferred_element_type=jnp.float32)
    for c in range(out_ref.shape[0]):
        out_ref[c] = picked[:PAIRS].astype(out_ref.dtype)


def partials_kernel(
    lengths_ref, cache_lengths_ref, seq_ref, rows_ref, qd_ref, k_ref, v_ref, ck_ref, cv_ref,
    out_ref, q_scratch,
):
    tokens = k_ref.shape[0]
    cache_count = ck_ref.shape[1]
    ends = ends_of(lengths_ref)
    q_scratch[...] = jnp.zeros_like(q_scratch)
    for g in range(GROUP):
        q_scratch[g * SLOT : g * SLOT + PAIRS, :] = rows_ref[
            :, g * HD : (g + 1) * HD
        ].astype(jnp.float32)
        q_scratch[g * SLOT + PAIRS : g * SLOT + ROWS, :] = qd_ref[
            :, g * HD : (g + 1) * HD
        ].astype(jnp.float32)
    queries = q_scratch[...].astype(jnp.bfloat16)
    keys = jnp.concatenate([k_ref[...], ck_ref[...].reshape(PROMPTS * cache_count, HD)], axis=0)
    values = jnp.concatenate([v_ref[...], cv_ref[...].reshape(PROMPTS * cache_count, HD)], axis=0)
    count = tokens + PROMPTS * cache_count
    scores = lax.dot_general(queries, keys, NT, preferred_element_type=jnp.float32) * score_scale
    lane = lax.broadcasted_iota(jnp.int32, (1, count), 1)
    key_pos = lane + seq_ref[0] * tokens
    key_seg = jnp.zeros((1, count), jnp.int32)
    for p in range(PAIRS):
        key_seg = key_seg + jnp.where(key_pos >= ends[p], 1, 0)
    owner = key_seg
    for p in range(PROMPTS):
        first = tokens + p * cache_count
        mine = (lane >= first) & (lane < first + cache_count)
        cache_pos = lane - first + seq_ref[0] * cache_count
        label = jnp.where(cache_pos < cache_lengths_ref[p], PAIRS + p, -1)
        owner = jnp.where(mine, label, owner)
    item = lax.broadcasted_iota(jnp.int32, (GROUP * SLOT, count), 0) % SLOT
    visible = item == owner
    scores = jnp.where(visible, scores, masked_score)
    top = jnp.max(scores, axis=1, keepdims=True)
    terms = jnp.where(visible, jnp.exp(scores - top), 0.0)
    total = jnp.sum(terms, axis=1, keepdims=True)
    sums = jnp.dot(terms.astype(jnp.bfloat16), values, preferred_element_type=jnp.float32)
    put_partials(out_ref, sums, top, total)


def three_parts(x):
    high = x.astype(jnp.bfloat16).astype(jnp.float32)
    middle = (x - high).astype(jnp.bfloat16).astype(jnp.float32)
    return high, middle, x - high - middle


def put_partials(out_ref, sums, top, total):
    across = (GROUP * SLOT, HD)
    row = lax.broadcasted_iota(jnp.int32, across, 0)
    packed = sums
    for first, column in ((ROWS, top), (SLOT + ROWS, total)):
        lanes = jnp.transpose(jnp.broadcast_to(column, across))[:1]
        lanes = jnp.concatenate([lanes, jnp.zeros_like(lanes)], axis=1)
        for j, part in enumerate(three_parts(lanes)):
            packed = jnp.where(row == first + j, part, packed)
    packed = packed.astype(out_ref.dtype)
    for c in range(out_ref.shape[0]):
        out_ref[c] = packed


def merged(pieces_ref):
    count = pieces_ref.shape[0]
    pieces = [pieces_ref[c].astype(jnp.float32) for c in range(count)]

    def columns(first):
        lines = [
            jnp.sum(piece[first : first + 3], axis=0, keepdims=True) for piece in pieces
        ] + [jnp.zeros((8 - count % 8, HD), jnp.float32)] * (count % 8 > 0)
        turned = jnp.transpose(jnp.concatenate(lines, axis=0))[: GROUP * SLOT]
        return [turned[:, c : c + 1] for c in range(count)]

    tops, totals = columns(ROWS), columns(SLOT + ROWS)
    top = functools.reduce(jnp.maximum, tops)
    total = jnp.zeros_like(top)
    sums = jnp.zeros((GROUP * SLOT, HD), jnp.float32)
    for c in range(count):
        scale = jnp.exp(tops[c] - top)
        total = total + totals[c] * scale
        sums = sums + pieces[c] * scale
    return sums, top, total


def merge_kernel(pieces_ref, out_ref):
    put_partials(out_ref, *merged(pieces_ref))


def table_kernel(ids_ref, tp_ref, after_ref, table_ref, out_ref, blocks, sems):
    vocab_rows, width = table_ref.shape
    picks = []
    for c in range(2):
        for r in range(ROWS):
            local = ids_ref[r, c] - tp_ref[0] * vocab_rows
            inside = (local >= 0) & (local < vocab_rows)
            local = jnp.clip(local, 0, vocab_rows - 1)
            picks.append((jnp.where(inside, local % TABLE_ROWS, -1), local // TABLE_ROWS))
    copies = []
    for i, (_, block) in enumerate(picks):
        rows = pl.ds(pl.multiple_of(block * TABLE_ROWS, TABLE_ROWS), TABLE_ROWS)
        copies.append(pltpu.make_async_copy(table_ref.at[rows], blocks.at[i], sems.at[i]))
        copies[-1].start()
    for copy in copies:
        copy.wait()
    index = lax.broadcasted_iota(jnp.int32, (TABLE_ROWS, width), 0)
    for i, (row, _) in enumerate(picks):
        block = jnp.where(index == row, blocks[i].astype(jnp.float32), 0.0)
        out_ref[i : i + 1, :] = jnp.sum(block, axis=0, keepdims=True)


def project_kernel(pieces_ref, w_ref, table_ref, out_ref):
    sums, _, total = merged(pieces_ref)
    rows = sums / total
    partial = jnp.zeros((SLOT, w_ref.shape[1]), jnp.float32)
    for g in range(GROUP):
        partial = partial + jnp.dot(
            rows[g * SLOT : (g + 1) * SLOT].astype(jnp.bfloat16),
            w_ref[g * HD : (g + 1) * HD, :],
            preferred_element_type=jnp.float32,
        )
    for c in range(out_ref.shape[0]):
        out_ref[c, :ROWS] = partial[:ROWS]
        out_ref[c, ROWS:] = table_ref[...]


def residual_kernel(pieces_ref, stream_ref, gain_ref, gained_ref, sums_ref):
    total = pieces_ref[0]
    for c in range(1, pieces_ref.shape[0]):
        total = total + pieces_ref[c]
    table = total[ROWS:]
    residual = total[:ROWS] + stream_ref[...].astype(jnp.float32)
    gained = residual * gain_ref[...].astype(jnp.float32)
    gained_ref[...] = gained
    squares = jnp.sum(residual * residual, axis=1, keepdims=True)
    first = jnp.sum(gained * table[:ROWS], axis=1, keepdims=True)
    second = jnp.sum(gained * table[ROWS:], axis=1, keepdims=True)
    lane = lax.broadcasted_iota(jnp.int32, (ROWS, HD), 1)
    packed = jnp.where(lane == 0, squares, jnp.where(lane == 1, first, second))
    packed = jnp.concatenate([packed, jnp.zeros((HD - ROWS, HD), jnp.float32)], axis=0)
    packed = jnp.transpose(packed)[:8]
    for c in range(sums_ref.shape[0]):
        sums_ref[c] = packed


def verdict_kernel(sums_ref, gained_ref, hidden_ref, win_ref):
    sums = jnp.transpose(sums_ref[...])[:ROWS]
    inv_rms = 1.0 / jnp.sqrt(sums[:, 0:1] / D + norm_eps)
    hidden_ref[...] = (gained_ref[...] * inv_rms).astype(hidden_ref.dtype)
    win = 1.0 / (1.0 + jnp.exp((sums[:, 2:3] - sums[:, 1:2]) * inv_rms))
    win_ref[...] = jnp.broadcast_to(win, win_ref.shape)


def attention_kernel(
    lengths_ref, seq_ref, q_hbm, kv_ref, out_ref, q_ref, kv_buf, top_ref, total_ref, sum_ref,
    q_sem, sems,
):
    tokens = q_ref.shape[0]
    q_copy = pltpu.make_async_copy(q_hbm, q_ref, q_sem)
    q_copy.start()
    first = seq_ref[0] * tokens
    ends = ends_of(lengths_ref)
    start_first = jnp.int32(0)
    start_last = jnp.int32(0)
    for p in range(PAIRS):
        start_first = jnp.where(ends[p] <= first, ends[p], start_first)
        start_last = jnp.where(ends[p] <= first + tokens - 1, ends[p], start_last)
    low = start_first // KEY_BLOCK
    high = (first + tokens + KEY_BLOCK - 1) // KEY_BLOCK

    def fetch(b):
        rows = pl.ds(pl.multiple_of(b * KEY_BLOCK, KEY_BLOCK), KEY_BLOCK)
        return pltpu.make_async_copy(kv_ref.at[rows], kv_buf.at[rows], sems.at[b])

    def begin(b, carry):
        fetch(b).start()
        return carry

    lax.fori_loop(low, high, begin, 0)
    top_ref[...] = jnp.full_like(top_ref, masked_score)
    total_ref[...] = jnp.zeros_like(total_ref)
    sum_ref[...] = jnp.zeros_like(sum_ref)
    query_pos = lax.broadcasted_iota(jnp.int32, (1, tokens), 1) + first
    query_start = jnp.zeros((1, tokens), jnp.int32)
    for p in range(PAIRS):
        query_start = jnp.where(query_pos >= ends[p], ends[p], query_start)

    def attend(b, masked):
        key_first = b * KEY_BLOCK
        rows = pl.ds(pl.multiple_of(key_first, KEY_BLOCK), KEY_BLOCK)
        keys = kv_buf[rows, :HD]
        values = jnp.transpose(kv_buf[rows, HD:])
        if masked:
            key_pos = lax.broadcasted_iota(jnp.int32, (KEY_BLOCK, tokens), 0) + key_first
            visible = (key_pos >= query_start) & (key_pos <= query_pos)
        for g in range(GROUP):
            queries = q_ref[:, g * HD : (g + 1) * HD]
            scores = lax.dot_general(keys, queries, NT, preferred_element_type=jnp.float32)
            if masked:
                scores = jnp.where(visible, scores, masked_score)
            old_top = top_ref[g]
            tops = jnp.max(scores.reshape(KEY_BLOCK // 8, 8, tokens), axis=0)
            new_top = jnp.maximum(old_top, jnp.max(tops, axis=0, keepdims=True))
            rescale = jnp.exp2((old_top - new_top) * exp2_scale)
            terms = jnp.exp2((scores - new_top) * exp2_scale)
            sums = jnp.sum(terms.reshape(KEY_BLOCK // 8, 8, tokens), axis=0)
            total_ref[g] = total_ref[g] * rescale + sums
            sum_ref[g] = sum_ref[g] * rescale + jnp.dot(
                values, terms.astype(jnp.bfloat16), preferred_element_type=jnp.float32
            )
            top_ref[g] = new_top

    def step(b, carry):
        fetch(b).wait()
        key_first = b * KEY_BLOCK
        masked = (key_first < start_last) | (key_first + KEY_BLOCK > first + 1)

        @pl.when(masked)
        def _():
            attend(b, True)

        @pl.when(jnp.logical_not(masked))
        def _():
            attend(b, False)

        return carry

    q_copy.wait()
    lax.fori_loop(low, high, step, 0)
    for g in range(GROUP):
        total = jnp.sum(total_ref[g], axis=0, keepdims=True)
        rows = jnp.transpose(sum_ref[g] / total)
        out_ref[:, g * HD : (g + 1) * HD] = rows.astype(out_ref.dtype)


def attention(lengths, seq_index, q, kv):
    tokens = q.shape[0]
    return pl.pallas_call(
        attention_kernel,
        out_shape=jax.ShapeDtypeStruct(q.shape, q.dtype),
        in_specs=[SM, SM, HB, HB],
        out_specs=VM,
        scratch_shapes=[
            pltpu.VMEM(q.shape, q.dtype),
            pltpu.VMEM(kv.shape, kv.dtype),
            pltpu.VMEM((GROUP, 1, tokens), jnp.float32),
            pltpu.VMEM((GROUP, 8, tokens), jnp.float32),
            pltpu.VMEM((GROUP, HD, tokens), jnp.float32),
            pltpu.SemaphoreType.DMA,
            pltpu.SemaphoreType.DMA((kv.shape[0] // KEY_BLOCK,)),
        ],
        compiler_params=pltpu.CompilerParams(vmem_limit_bytes=24 * 1024 * 1024),
        name="attention",
    )(lengths, seq_index, held(q), held(kv))


def call(kernel, shapes, specs, name, scratch=()):
    many = isinstance(shapes, tuple)
    return pl.pallas_call(
        kernel,
        out_shape=shapes,
        in_specs=specs,
        out_specs=tuple(VM for _ in shapes) if many else VM,
        scratch_shapes=list(scratch),
        compiler_params=pltpu.CompilerParams(vmem_limit_bytes=8 * 1024 * 1024),
        name=name,
    )


def shards(
    q_prefill,
    k_prefill,
    v_prefill,
    pair_lengths,
    q_decode,
    cache_k,
    cache_v,
    cache_lengths,
    stream,
    out_weight,
    norm_gain,
    vocab_table,
    verdict_ids,
):
    f32 = jnp.float32
    lo = lax.axis_size("seq_lo")
    hi = lax.axis_size("seq_hi")
    tp = lax.axis_size(TP)
    columns = q_prefill.shape[1]
    width = stream.shape[1]
    pair_lengths, cache_lengths = held(pair_lengths), held(cache_lengths)
    seq_index = lax.axis_index(SEQ).astype(jnp.int32).reshape(1)
    shape = jax.ShapeDtypeStruct

    picked, kv = call(
        last_rows_kernel,
        (
            shape((lo, PAIRS, columns), jnp.bfloat16),
            shape((q_prefill.shape[0], 2 * HD), jnp.bfloat16),
        ),
        [SM, SM, PIPE, PIPE, PIPE],
        "last_rows",
    )(pair_lengths, seq_index, held(q_prefill), held(k_prefill), held(v_prefill))
    kv = lax.all_gather(kv, SEQ, axis=0, tiled=True)
    rows = jnp.sum(exchanged(picked, "seq_lo").astype(f32), axis=0)
    rows = lax.psum(rows.astype(jnp.bfloat16), "seq_hi")

    partials = call(
        partials_kernel,
        shape((lo, GROUP * SLOT, HD), jnp.bfloat16),
        [SM, SM, SM, VM] + [PIPE] * 5,
        "partials",
        [pltpu.VMEM((GROUP * SLOT, HD), f32)],
    )(
        pair_lengths, cache_lengths, seq_index, rows, held(q_decode), held(k_prefill),
        held(v_prefill), held(cache_k), held(cache_v),
    )
    partials = exchanged(partials, "seq_lo")
    merged_rows = call(merge_kernel, shape((hi, GROUP * SLOT, HD), jnp.bfloat16), [VM], "merge")(
        partials
    )
    partials = exchanged(merged_rows, "seq_hi")

    tp_index = lax.axis_index(TP).astype(jnp.int32).reshape(1)
    table_rows = call(
        table_kernel,
        shape((2 * ROWS, width), f32),
        [SM, SM, HB, HB],
        "table",
        [
            pltpu.VMEM((2 * ROWS, TABLE_ROWS, width), jnp.bfloat16),
            pltpu.SemaphoreType.DMA((2 * ROWS,)),
        ],
    )(verdict_ids, tp_index, merged_rows, held(vocab_table))
    pieces = call(
        project_kernel, shape((tp, 3 * ROWS, width), f32), [VM, PIPE, VM], "project"
    )(partials, held(out_weight), table_rows)
    pieces = exchanged(pieces, TP)
    gained, sums = call(
        residual_kernel,
        (shape((ROWS, width), f32), shape((lo, 8, HD), f32)),
        [VM, PIPE, PIPE],
        "residual",
    )(pieces, held(stream), held(norm_gain.reshape(1, width)))
    sums = jnp.sum(exchanged(sums, "seq_lo"), axis=0)
    sums = lax.psum(sums, "seq_hi")
    verdict_hidden, win = call(
        verdict_kernel,
        (shape((ROWS, width), jnp.bfloat16), shape((ROWS, HD), f32)),
        [VM, VM],
        "verdict",
    )(sums, gained)

    attended = attention(pair_lengths, seq_index, q_prefill, kv)
    return (attended, verdict_hidden, win[:, 0])


def solution(mesh):
    groups, seq = mesh.shape["groups"], mesh.shape["seq"]
    torus = Mesh(
        mesh.devices.reshape(groups, seq // LO, LO, mesh.shape["tp"] // 2, 2),
        ("groups",) + SEQ + TP,
    )
    tokens = ("groups",) + SEQ
    return jax.shard_map(
        shards,
        mesh=torus,
        in_specs=(
            P(tokens, TP),
            P(tokens, TP),
            P(tokens, TP),
            P("groups"),
            P("groups", TP),
            P("groups", SEQ, TP),
            P("groups", SEQ, TP),
            P("groups"),
            P("groups", SEQ),
            P(TP, SEQ),
            P(SEQ),
            P(TP, SEQ),
            P("groups", None),
        ),
        out_specs=(P(tokens, TP), P("groups", SEQ), P("groups")),
        check_vma=False,
    )
```

```python
import functools

import jax
import jax.numpy as jnp
from jax import lax
from jax.experimental import pallas as pl
from jax.experimental.pallas import tpu as pltpu
from jax.sharding import Mesh
from jax.sharding import PartitionSpec as P

D = 8192
H = 32
KVH = 8
HD = 128
PROMPTS = 4
PAIRS = 8
ROWS = 12
GROUP = H // KVH
LO = 8
SLOT = 16
PART = 8
HELD = 6
KEY_BLOCK = 256
TP = ("tp_0", "tp_1")
SEQ = ("seq_hi", "seq_lo")

masked_score = -1e30
norm_eps = 1e-05
score_scale = 1.0 / HD**0.5
exp2_scale = score_scale * 1.4426950408889634

NT = (((1,), (1,)), ((), ()))
VM = pl.BlockSpec(memory_space=pltpu.VMEM)
SM = pl.BlockSpec(memory_space=pltpu.SMEM)
HB = pl.BlockSpec(memory_space=pltpu.HBM)
PIPE = pl.BlockSpec()
TABLE_ROWS = 16


def held(x):
    return pltpu.with_memory_space_constraint(x, pltpu.HBM)


def exchanged(copies, axis):
    return lax.all_to_all(copies, axis, 0, 0, tiled=True)


def ends_of(lengths_ref):
    ends, total = [], 0
    for p in range(PAIRS):
        total = total + lengths_ref[p]
        ends.append(total)
    return ends


def last_rows_kernel(lengths_ref, seq_ref, q_ref, k_ref, v_ref, out_ref, kv_ref):
    kv_ref[:, :HD] = k_ref[...]
    kv_ref[:, HD:] = v_ref[...]
    tokens = q_ref.shape[0]
    ends = ends_of(lengths_ref)
    row = lax.broadcasted_iota(jnp.int32, (SLOT, tokens), 0)
    col = lax.broadcasted_iota(jnp.int32, (SLOT, tokens), 1) + seq_ref[0] * tokens
    last = jnp.full((SLOT, tokens), -1, jnp.int32)
    for p in range(PAIRS):
        last = jnp.where(row == p, ends[p] - 1, last)
    selector = jnp.where(col == last, 1.0, 0.0).astype(jnp.bfloat16)
    picked = jnp.dot(selector, q_ref[...], preferred_element_type=jnp.float32)
    for c in range(out_ref.shape[0]):
        out_ref[c] = picked[:PAIRS].astype(out_ref.dtype)


def table_copies(ids_ref, tp_ref, table_ref, blocks, sems):
    vocab_rows = table_ref.shape[0]
    copies, places = [], []
    for c in range(2):
        for r in range(ROWS):
            local = ids_ref[r, c] - tp_ref[0] * vocab_rows
            inside = (local >= 0) & (local < vocab_rows)
            local = jnp.clip(local, 0, vocab_rows - 1)
            places.append(jnp.where(inside, local % TABLE_ROWS, -1))
            first = pl.multiple_of(local // TABLE_ROWS * TABLE_ROWS, TABLE_ROWS)
            i = len(copies)
            copies.append(
                pltpu.make_async_copy(
                    table_ref.at[pl.ds(first, TABLE_ROWS)], blocks.at[i], sems.at[i]
                )
            )
    return copies, places


def spread(columns):
    row = lax.broadcasted_iota(jnp.int32, (PART, HD), 0)
    lane = lax.broadcasted_iota(jnp.int32, (PART, HD), 1)
    line = jnp.zeros((PART, HD), jnp.float32)
    for j, column in enumerate(columns):
        line = jnp.where(lane == j * PART + row, column, line)
    return jnp.sum(line, axis=0, keepdims=True)


def gathered(line, first, count):
    row = lax.broadcasted_iota(jnp.int32, (PART, HD), 0)
    lane = lax.broadcasted_iota(jnp.int32, (PART, HD), 1)
    wanted = (lane % PART == row) & (lane >= first * PART) & (lane < (first + count) * PART)
    return jnp.sum(jnp.where(wanted, line, 0.0), axis=1, keepdims=True)


def three_parts(x):
    high = x.astype(jnp.bfloat16).astype(jnp.float32)
    middle = (x - high).astype(jnp.bfloat16).astype(jnp.float32)
    return high, middle, x - high - middle


def partials_kernel(
    lengths_ref, cache_lengths_ref, seq_ref, ids_ref, tp_ref, rows_ref, qd_ref, k_ref, v_ref,
    ck_ref, cv_ref, table_ref, out_ref, picked_ref, q_scratch, blocks, sems,
):
    copies, places = table_copies(ids_ref, tp_ref, table_ref, blocks, sems)
    for copy in copies:
        copy.start()
    tokens = k_ref.shape[0]
    cache_count = ck_ref.shape[1]
    ends = ends_of(lengths_ref)
    q_scratch[...] = jnp.zeros_like(q_scratch)
    for g in range(GROUP):
        columns = slice(g * HD, (g + 1) * HD)
        base, next_part = g * SLOT, g * SLOT + PART
        both = PAIRS - HELD
        pair_rows = rows_ref[:, columns].astype(jnp.float32)
        q_scratch[base : base + HELD, :] = pair_rows[:HELD]
        q_scratch[next_part : next_part + both, :] = pair_rows[HELD:]
        q_scratch[next_part + both : next_part + HELD, :] = qd_ref[:, columns].astype(jnp.float32)
    queries = q_scratch[...].astype(jnp.bfloat16)
    keys = jnp.concatenate([k_ref[...], ck_ref[...].reshape(PROMPTS * cache_count, HD)], axis=0)
    values = jnp.concatenate([v_ref[...], cv_ref[...].reshape(PROMPTS * cache_count, HD)], axis=0)
    count = tokens + PROMPTS * cache_count
    scores = lax.dot_general(queries, keys, NT, preferred_element_type=jnp.float32) * score_scale
    lane = lax.broadcasted_iota(jnp.int32, (1, count), 1)
    key_pos = lane + seq_ref[0] * tokens
    key_seg = jnp.zeros((1, count), jnp.int32)
    for p in range(PAIRS):
        key_seg = key_seg + jnp.where(key_pos >= ends[p], 1, 0)
    owner = key_seg
    for p in range(PROMPTS):
        first = tokens + p * cache_count
        mine = (lane >= first) & (lane < first + cache_count)
        cache_pos = lane - first + seq_ref[0] * cache_count
        label = jnp.where(cache_pos < cache_lengths_ref[p], PAIRS + p, -1)
        owner = jnp.where(mine, label, owner)
    row = lax.broadcasted_iota(jnp.int32, (GROUP * SLOT, count), 0)
    item = jnp.where(row % PART < HELD, row % PART + row % SLOT // PART * HELD, -2)
    visible = item == owner
    scores = jnp.where(visible, scores, masked_score)
    top = jnp.max(scores, axis=1, keepdims=True)
    terms = jnp.where(visible, jnp.exp(scores - top), 0.0)
    total = jnp.sum(terms, axis=1, keepdims=True)
    sums = jnp.dot(terms.astype(jnp.bfloat16), values, preferred_element_type=jnp.float32)
    place = lax.broadcasted_iota(jnp.int32, (PART, HD), 0)
    for c in range(out_ref.shape[0]):
        rows = slice(c * PART, (c + 1) * PART)
        out_ref[c] = jnp.where(place == HELD, spread((top[rows], total[rows])), sums[rows])
    for copy in copies:
        copy.wait()
    index = lax.broadcasted_iota(jnp.int32, blocks.shape[1:], 0)
    for i, wanted in enumerate(places):
        block = jnp.where(index == wanted, blocks[i].astype(jnp.float32), 0.0)
        picked_ref[i : i + 1, :] = jnp.sum(block, axis=0, keepdims=True)


def merged(pieces, parts):
    tops = [gathered(piece[HELD : HELD + 1], 0, parts) for piece in pieces]
    totals = [gathered(piece[HELD : HELD + 1], parts, parts) for piece in pieces]
    top = functools.reduce(jnp.maximum, tops)
    total = jnp.zeros_like(top)
    sums = jnp.zeros((PART, HD), jnp.float32)
    for piece, piece_top, piece_total in zip(pieces, tops, totals):
        scale = jnp.exp(piece_top - top)
        total = total + piece_total * scale
        sums = sums + piece * scale
    return sums, top, total


def merge_kernel(hi_ref, pieces_ref, out_ref):
    sums, top, total = merged([pieces_ref[c] for c in range(pieces_ref.shape[0])], 1)
    row = lax.broadcasted_iota(jnp.int32, (PART, HD), 0)
    line = spread(three_parts(top) + three_parts(total))
    block = jnp.where(row == HELD, line, jnp.where(row < HELD, sums, 0.0))
    slots = [jnp.where(hi_ref[0] == k, block, 0.0) for k in range(out_ref.shape[0] // PART)]
    out_ref[...] = jnp.concatenate(slots, axis=0).astype(out_ref.dtype)


def finish_kernel(slots_ref, out_ref):
    slots = slots_ref[...].astype(jnp.float32)
    count = slots_ref.shape[0] // PART
    sums, _, total = merged([slots[k * PART : (k + 1) * PART] for k in range(count)], 3)
    row = lax.broadcasted_iota(jnp.int32, (PART, HD), 0)
    rows = jnp.where(row < HELD, sums / total, 0.0).astype(out_ref.dtype)
    for c in range(out_ref.shape[0]):
        out_ref[c] = rows


def project_kernel(parts_ref, w_ref, table_ref, out_ref):
    partial = jnp.zeros((SLOT, w_ref.shape[1]), jnp.float32)
    for g in range(GROUP):
        rows = [parts_ref[2 * g + j].astype(jnp.float32) for j in range(2)]
        partial = partial + jnp.dot(
            jnp.concatenate(rows, axis=0).astype(jnp.bfloat16),
            w_ref[g * HD : (g + 1) * HD, :],
            preferred_element_type=jnp.float32,
        )
    for c in range(out_ref.shape[0]):
        out_ref[c, :HELD] = partial[:HELD]
        out_ref[c, HELD:ROWS] = partial[PART : PART + HELD]
        out_ref[c, ROWS:] = table_ref[...]


def residual_kernel(pieces_ref, stream_ref, gain_ref, gained_ref, sums_ref):
    total = pieces_ref[0]
    for c in range(1, pieces_ref.shape[0]):
        total = total + pieces_ref[c]
    table = total[ROWS:]
    residual = total[:ROWS] + stream_ref[...].astype(jnp.float32)
    gained = residual * gain_ref[...].astype(jnp.float32)
    gained_ref[...] = gained
    squares = jnp.sum(residual * residual, axis=1, keepdims=True)
    first = jnp.sum(gained * table[:ROWS], axis=1, keepdims=True)
    second = jnp.sum(gained * table[ROWS:], axis=1, keepdims=True)
    lane = lax.broadcasted_iota(jnp.int32, (ROWS, HD), 1)
    packed = jnp.where(lane == 0, squares, jnp.where(lane == 1, first, second))
    packed = jnp.concatenate([packed, jnp.zeros((HD - ROWS, HD), jnp.float32)], axis=0)
    packed = jnp.transpose(packed)[:8]
    for c in range(sums_ref.shape[0]):
        sums_ref[c] = packed


def verdict_kernel(sums_ref, gained_ref, hidden_ref, win_ref):
    sums = jnp.transpose(sums_ref[...])[:ROWS]
    inv_rms = 1.0 / jnp.sqrt(sums[:, 0:1] / D + norm_eps)
    hidden_ref[...] = (gained_ref[...] * inv_rms).astype(hidden_ref.dtype)
    lines = sums_ref[...]
    inv_rms = 1.0 / jnp.sqrt(lines[0:1] / D + norm_eps)
    win = 1.0 / (1.0 + jnp.exp((lines[2:3] - lines[1:2]) * inv_rms))
    win_ref[...] = win[0, :ROWS]


def attention_kernel(
    lengths_ref, seq_ref, q_hbm, kv_ref, out_ref, q_ref, kv_buf, top_ref, total_ref, sum_ref,
    q_sem, sems,
):
    tokens = q_ref.shape[0]
    q_copy = pltpu.make_async_copy(q_hbm, q_ref, q_sem)
    q_copy.start()
    first = seq_ref[0] * tokens
    ends = ends_of(lengths_ref)
    start_first = jnp.int32(0)
    start_last = jnp.int32(0)
    for p in range(PAIRS):
        start_first = jnp.where(ends[p] <= first, ends[p], start_first)
        start_last = jnp.where(ends[p] <= first + tokens - 1, ends[p], start_last)
    low = start_first // KEY_BLOCK
    high = (first + tokens + KEY_BLOCK - 1) // KEY_BLOCK

    def fetch(b):
        rows = pl.ds(pl.multiple_of(b * KEY_BLOCK, KEY_BLOCK), KEY_BLOCK)
        return pltpu.make_async_copy(kv_ref.at[rows], kv_buf.at[rows], sems.at[b])

    def begin(b, carry):
        fetch(b).start()
        return carry

    lax.fori_loop(low, high, begin, 0)
    top_ref[...] = jnp.full_like(top_ref, masked_score)
    total_ref[...] = jnp.zeros_like(total_ref)
    sum_ref[...] = jnp.zeros_like(sum_ref)
    query_pos = lax.broadcasted_iota(jnp.int32, (1, tokens), 1) + first
    query_start = jnp.zeros((1, tokens), jnp.int32)
    for p in range(PAIRS):
        query_start = jnp.where(query_pos >= ends[p], ends[p], query_start)

    def attend(b, masked):
        key_first = b * KEY_BLOCK
        rows = pl.ds(pl.multiple_of(key_first, KEY_BLOCK), KEY_BLOCK)
        keys = kv_buf[rows, :HD]
        values = jnp.transpose(kv_buf[rows, HD:])
        if masked:
            key_pos = lax.broadcasted_iota(jnp.int32, (KEY_BLOCK, tokens), 0) + key_first
            visible = (key_pos >= query_start) & (key_pos <= query_pos)
        for g in range(GROUP):
            queries = q_ref[:, g * HD : (g + 1) * HD]
            scores = lax.dot_general(keys, queries, NT, preferred_element_type=jnp.float32)
            if masked:
                scores = jnp.where(visible, scores, masked_score)
            old_top = top_ref[g]
            tops = jnp.max(scores.reshape(KEY_BLOCK // 8, 8, tokens), axis=0)
            new_top = jnp.maximum(old_top, jnp.max(tops, axis=0, keepdims=True))
            rescale = jnp.exp2((old_top - new_top) * exp2_scale)
            terms = jnp.exp2((scores - new_top) * exp2_scale)
            sums = jnp.sum(terms.reshape(KEY_BLOCK // 8, 8, tokens), axis=0)
            total_ref[g] = total_ref[g] * rescale + sums
            sum_ref[g] = sum_ref[g] * rescale + jnp.dot(
                values, terms.astype(jnp.bfloat16), preferred_element_type=jnp.float32
            )
            top_ref[g] = new_top

    def step(b, carry):
        fetch(b).wait()
        key_first = b * KEY_BLOCK
        masked = (key_first < start_last) | (key_first + KEY_BLOCK > first + 1)

        @pl.when(masked)
        def _():
            attend(b, True)

        @pl.when(jnp.logical_not(masked))
        def _():
            attend(b, False)

        return carry

    q_copy.wait()
    lax.fori_loop(low, high, step, 0)
    for g in range(GROUP):
        total = jnp.sum(total_ref[g], axis=0, keepdims=True)
        rows = jnp.transpose(sum_ref[g] / total)
        out_ref[:, g * HD : (g + 1) * HD] = rows.astype(out_ref.dtype)


def attention(lengths, seq_index, q, kv):
    tokens = q.shape[0]
    return pl.pallas_call(
        attention_kernel,
        out_shape=jax.ShapeDtypeStruct(q.shape, q.dtype),
        in_specs=[SM, SM, HB, HB],
        out_specs=VM,
        scratch_shapes=[
            pltpu.VMEM(q.shape, q.dtype),
            pltpu.VMEM(kv.shape, kv.dtype),
            pltpu.VMEM((GROUP, 1, tokens), jnp.float32),
            pltpu.VMEM((GROUP, 8, tokens), jnp.float32),
            pltpu.VMEM((GROUP, HD, tokens), jnp.float32),
            pltpu.SemaphoreType.DMA,
            pltpu.SemaphoreType.DMA((kv.shape[0] // KEY_BLOCK,)),
        ],
        compiler_params=pltpu.CompilerParams(vmem_limit_bytes=24 * 1024 * 1024),
        name="attention",
    )(lengths, seq_index, held(q), held(kv))


def call(kernel, shapes, specs, name, scratch=()):
    many = isinstance(shapes, tuple)
    return pl.pallas_call(
        kernel,
        out_shape=shapes,
        in_specs=specs,
        out_specs=tuple(VM for _ in shapes) if many else VM,
        scratch_shapes=list(scratch),
        compiler_params=pltpu.CompilerParams(vmem_limit_bytes=8 * 1024 * 1024),
        name=name,
    )


def shards(
    q_prefill,
    k_prefill,
    v_prefill,
    pair_lengths,
    q_decode,
    cache_k,
    cache_v,
    cache_lengths,
    stream,
    out_weight,
    norm_gain,
    vocab_table,
    verdict_ids,
):
    f32 = jnp.float32
    lo = lax.axis_size("seq_lo")
    hi = lax.axis_size("seq_hi")
    tp = lax.axis_size(TP)
    columns = q_prefill.shape[1]
    width = stream.shape[1]
    pair_lengths, cache_lengths = held(pair_lengths), held(cache_lengths)
    seq_index = lax.axis_index(SEQ).astype(jnp.int32).reshape(1)
    shape = jax.ShapeDtypeStruct

    picked, kv = call(
        last_rows_kernel,
        (
            shape((lo, PAIRS, columns), jnp.bfloat16),
            shape((q_prefill.shape[0], 2 * HD), jnp.bfloat16),
        ),
        [SM, SM, PIPE, PIPE, PIPE],
        "last_rows",
    )(pair_lengths, seq_index, held(q_prefill), held(k_prefill), held(v_prefill))
    kv = lax.all_gather(kv, SEQ, axis=0, tiled=True)
    rows = jnp.sum(exchanged(picked, "seq_lo").astype(f32), axis=0)
    rows = lax.psum(rows.astype(jnp.bfloat16), "seq_hi")

    tp_index = lax.axis_index(TP).astype(jnp.int32).reshape(1)
    hi_index = lax.axis_index("seq_hi").astype(jnp.int32).reshape(1)
    partials, table_rows = call(
        partials_kernel,
        (shape((lo, PART, HD), f32), shape((2 * ROWS, width), f32)),
        [SM] * 5 + [VM] + [PIPE] * 5 + [HB],
        "partials",
        [
            pltpu.VMEM((GROUP * SLOT, HD), f32),
            pltpu.VMEM((2 * ROWS, TABLE_ROWS, width), jnp.bfloat16),
            pltpu.SemaphoreType.DMA((2 * ROWS,)),
        ],
    )(
        pair_lengths, cache_lengths, seq_index, verdict_ids, tp_index, rows, held(q_decode),
        held(k_prefill), held(v_prefill), held(cache_k), held(cache_v), held(vocab_table),
    )
    slots = call(merge_kernel, shape((hi * PART, HD), jnp.bfloat16), [SM, VM], "merge")(
        hi_index, exchanged(partials, "seq_lo")
    )
    slots = lax.psum(slots, "seq_hi")
    parts = call(finish_kernel, shape((lo, PART, HD), jnp.bfloat16), [VM], "finish")(slots)
    parts = exchanged(parts, "seq_lo")
    pieces = call(
        project_kernel, shape((tp, 3 * ROWS, width), f32), [VM, PIPE, VM], "project"
    )(parts, held(out_weight), table_rows)
    pieces = exchanged(pieces, TP)
    gained, sums = call(
        residual_kernel,
        (shape((ROWS, width), f32), shape((lo, 8, HD), f32)),
        [VM, PIPE, PIPE],
        "residual",
    )(pieces, held(stream), held(norm_gain.reshape(1, width)))
    sums = jnp.sum(exchanged(sums, "seq_lo"), axis=0)
    sums = lax.psum(sums, "seq_hi")
    verdict_hidden, win = call(
        verdict_kernel,
        (shape((ROWS, width), jnp.bfloat16), shape((ROWS,), f32)),
        [VM, VM],
        "verdict",
    )(sums, gained)

    attended = attention(pair_lengths, seq_index, q_prefill, kv)
    return (attended, verdict_hidden, win)


def solution(mesh):
    groups, seq = mesh.shape["groups"], mesh.shape["seq"]
    torus = Mesh(
        mesh.devices.reshape(groups, seq // LO, LO, mesh.shape["tp"] // 2, 2),
        ("groups",) + SEQ + TP,
    )
    tokens = ("groups",) + SEQ
    return jax.shard_map(
        shards,
        mesh=torus,
        in_specs=(
            P(tokens, TP),
            P(tokens, TP),
            P(tokens, TP),
            P("groups"),
            P("groups", TP),
            P("groups", SEQ, TP),
            P("groups", SEQ, TP),
            P("groups"),
            P("groups", SEQ),
            P(TP, SEQ),
            P(SEQ),
            P(TP, SEQ),
            P("groups", None),
        ),
        out_specs=(P(tokens, TP), P("groups", SEQ), P("groups")),
        check_vma=False,
    )
```

```python
import functools

import jax
import jax.numpy as jnp
from jax import lax
from jax.experimental import pallas as pl
from jax.experimental.pallas import tpu as pltpu
from jax.sharding import Mesh
from jax.sharding import PartitionSpec as P

D = 8192
H = 32
KVH = 8
HD = 128
PROMPTS = 4
PAIRS = 8
ROWS = 12
GROUP = H // KVH
LO = 8
SLOT = 16
PART = 8
HELD = 6
KEY_BLOCK = 256
TP = ("tp_0", "tp_1")
SEQ = ("seq_hi", "seq_lo")

masked_score = -1e30
norm_eps = 1e-05
score_scale = 1.0 / HD**0.5
exp2_scale = score_scale * 1.4426950408889634

NT = (((1,), (1,)), ((), ()))
VM = pl.BlockSpec(memory_space=pltpu.VMEM)
SM = pl.BlockSpec(memory_space=pltpu.SMEM)
HB = pl.BlockSpec(memory_space=pltpu.HBM)
PIPE = pl.BlockSpec()
TABLE_ROWS = 16


def held(x):
    return pltpu.with_memory_space_constraint(x, pltpu.HBM)


def exchanged(copies, axis):
    return lax.all_to_all(copies, axis, 0, 0, tiled=True)


def ends_of(lengths_ref):
    ends, total = [], 0
    for p in range(PAIRS):
        total = total + lengths_ref[p]
        ends.append(total)
    return ends


def last_rows_kernel(lengths_ref, seq_ref, q_ref, k_ref, v_ref, out_ref, kv_ref):
    kv_ref[:, :HD] = k_ref[...]
    kv_ref[:, HD:] = v_ref[...]
    tokens = q_ref.shape[0]
    ends = ends_of(lengths_ref)
    row = lax.broadcasted_iota(jnp.int32, (SLOT, tokens), 0)
    col = lax.broadcasted_iota(jnp.int32, (SLOT, tokens), 1) + seq_ref[0] * tokens
    last = jnp.full((SLOT, tokens), -1, jnp.int32)
    for p in range(PAIRS):
        last = jnp.where(row == p, ends[p] - 1, last)
    selector = jnp.where(col == last, 1.0, 0.0).astype(jnp.bfloat16)
    picked = jnp.dot(selector, q_ref[...], preferred_element_type=jnp.float32)
    for c in range(out_ref.shape[0]):
        out_ref[c] = picked[:PAIRS].astype(out_ref.dtype)


def table_copies(ids_ref, tp_ref, table_ref, blocks, sems):
    vocab_rows = table_ref.shape[0]
    copies, places = [], []
    for c in range(2):
        for r in range(ROWS):
            local = ids_ref[c, r] - tp_ref[0] * vocab_rows
            inside = (local >= 0) & (local < vocab_rows)
            local = jnp.clip(local, 0, vocab_rows - 1)
            places.append(jnp.where(inside, local % TABLE_ROWS, -1))
            first = pl.multiple_of(local // TABLE_ROWS * TABLE_ROWS, TABLE_ROWS)
            i = len(copies)
            copies.append(
                pltpu.make_async_copy(
                    table_ref.at[pl.ds(first, TABLE_ROWS)], blocks.at[i], sems.at[i]
                )
            )
    return copies, places


def spread(columns):
    row = lax.broadcasted_iota(jnp.int32, (PART, HD), 0)
    lane = lax.broadcasted_iota(jnp.int32, (PART, HD), 1)
    line = jnp.zeros((PART, HD), jnp.float32)
    for j, column in enumerate(columns):
        line = jnp.where(lane == j * PART + row, column, line)
    return jnp.sum(line, axis=0, keepdims=True)


def gathered(line, first, count):
    row = lax.broadcasted_iota(jnp.int32, (PART, HD), 0)
    lane = lax.broadcasted_iota(jnp.int32, (PART, HD), 1)
    wanted = (lane % PART == row) & (lane >= first * PART) & (lane < (first + count) * PART)
    return jnp.sum(jnp.where(wanted, line, 0.0), axis=1, keepdims=True)


def three_parts(x):
    high = x.astype(jnp.bfloat16).astype(jnp.float32)
    middle = (x - high).astype(jnp.bfloat16).astype(jnp.float32)
    return high, middle, x - high - middle


def partials_kernel(
    lengths_ref, cache_lengths_ref, seq_ref, ids_ref, tp_ref, rows_ref, qd_ref, k_ref, v_ref,
    ck_ref, cv_ref, table_ref, out_ref, picked_ref, q_scratch, blocks, sems,
):
    copies, places = table_copies(ids_ref, tp_ref, table_ref, blocks, sems)
    for copy in copies:
        copy.start()
    tokens = k_ref.shape[0]
    cache_count = ck_ref.shape[1]
    ends = ends_of(lengths_ref)
    q_scratch[...] = jnp.zeros_like(q_scratch)
    for g in range(GROUP):
        columns = slice(g * HD, (g + 1) * HD)
        base, next_part = g * SLOT, g * SLOT + PART
        both = PAIRS - HELD
        pair_rows = rows_ref[:, columns].astype(jnp.float32)
        q_scratch[base : base + HELD, :] = pair_rows[:HELD]
        q_scratch[next_part : next_part + both, :] = pair_rows[HELD:]
        q_scratch[next_part + both : next_part + HELD, :] = qd_ref[:, columns].astype(jnp.float32)
    queries = q_scratch[...].astype(jnp.bfloat16)
    keys = jnp.concatenate([k_ref[...], ck_ref[...].reshape(PROMPTS * cache_count, HD)], axis=0)
    values = jnp.concatenate([v_ref[...], cv_ref[...].reshape(PROMPTS * cache_count, HD)], axis=0)
    count = tokens + PROMPTS * cache_count
    scores = lax.dot_general(queries, keys, NT, preferred_element_type=jnp.float32) * score_scale
    lane = lax.broadcasted_iota(jnp.int32, (1, count), 1)
    key_pos = lane + seq_ref[0] * tokens
    key_seg = jnp.zeros((1, count), jnp.int32)
    for p in range(PAIRS):
        key_seg = key_seg + jnp.where(key_pos >= ends[p], 1, 0)
    owner = key_seg
    for p in range(PROMPTS):
        first = tokens + p * cache_count
        mine = (lane >= first) & (lane < first + cache_count)
        cache_pos = lane - first + seq_ref[0] * cache_count
        label = jnp.where(cache_pos < cache_lengths_ref[p], PAIRS + p, -1)
        owner = jnp.where(mine, label, owner)
    row = lax.broadcasted_iota(jnp.int32, (GROUP * SLOT, count), 0)
    item = jnp.where(row % PART < HELD, row % PART + row % SLOT // PART * HELD, -2)
    visible = item == owner
    scores = jnp.where(visible, scores, masked_score)
    top = jnp.max(scores, axis=1, keepdims=True)
    terms = jnp.where(visible, jnp.exp(scores - top), 0.0)
    total = jnp.sum(terms, axis=1, keepdims=True)
    sums = jnp.dot(terms.astype(jnp.bfloat16), values, preferred_element_type=jnp.float32)
    place = lax.broadcasted_iota(jnp.int32, (PART, HD), 0)
    for c in range(out_ref.shape[0]):
        rows = slice(c * PART, (c + 1) * PART)
        out_ref[c] = jnp.where(place == HELD, spread((top[rows], total[rows])), sums[rows])
    for copy in copies:
        copy.wait()
    index = lax.broadcasted_iota(jnp.int32, blocks.shape[1:], 0)
    for i, wanted in enumerate(places):
        block = jnp.where(index == wanted, blocks[i].astype(jnp.float32), 0.0)
        picked_ref[i : i + 1, :] = jnp.sum(block, axis=0, keepdims=True)


def merged(pieces, parts):
    tops = [gathered(piece[HELD : HELD + 1], 0, parts) for piece in pieces]
    totals = [gathered(piece[HELD : HELD + 1], parts, parts) for piece in pieces]
    top = functools.reduce(jnp.maximum, tops)
    total = jnp.zeros_like(top)
    sums = jnp.zeros((PART, HD), jnp.float32)
    for piece, piece_top, piece_total in zip(pieces, tops, totals):
        scale = jnp.exp(piece_top - top)
        total = total + piece_total * scale
        sums = sums + piece * scale
    return sums, top, total


def merge_kernel(hi_ref, pieces_ref, out_ref):
    sums, top, total = merged([pieces_ref[c] for c in range(pieces_ref.shape[0])], 1)
    row = lax.broadcasted_iota(jnp.int32, (PART, HD), 0)
    line = spread(three_parts(top) + three_parts(total))
    block = jnp.where(row == HELD, line, jnp.where(row < HELD, sums, 0.0))
    slots = [jnp.where(hi_ref[0] == k, block, 0.0) for k in range(out_ref.shape[0] // PART)]
    out_ref[...] = jnp.concatenate(slots, axis=0).astype(out_ref.dtype)


def finish_kernel(slots_ref, out_ref):
    slots = slots_ref[...].astype(jnp.float32)
    count = slots_ref.shape[0] // PART
    sums, _, total = merged([slots[k * PART : (k + 1) * PART] for k in range(count)], 3)
    row = lax.broadcasted_iota(jnp.int32, (PART, HD), 0)
    rows = jnp.where(row < HELD, sums / total, 0.0).astype(out_ref.dtype)
    for c in range(out_ref.shape[0]):
        out_ref[c] = rows


def project_kernel(parts_ref, w_ref, table_ref, out_ref):
    partial = jnp.zeros((SLOT, w_ref.shape[1]), jnp.float32)
    for g in range(GROUP):
        rows = [parts_ref[2 * g + j].astype(jnp.float32) for j in range(2)]
        partial = partial + jnp.dot(
            jnp.concatenate(rows, axis=0).astype(jnp.bfloat16),
            w_ref[g * HD : (g + 1) * HD, :],
            preferred_element_type=jnp.float32,
        )
    both = jnp.concatenate(
        [partial[:HELD], partial[PART : PART + HELD], table_ref[...]], axis=0
    ).astype(out_ref.dtype)
    for c in range(out_ref.shape[0]):
        out_ref[c] = both


def residual_kernel(pieces_ref, stream_ref, gain_ref, gained_ref, sums_ref):
    total = pieces_ref[0].astype(jnp.float32)
    for c in range(1, pieces_ref.shape[0]):
        total = total + pieces_ref[c].astype(jnp.float32)
    table = total[ROWS:]
    residual = total[:ROWS] + stream_ref[...].astype(jnp.float32)
    gained = residual * gain_ref[...].astype(jnp.float32)
    gained_ref[...] = gained
    squares = jnp.sum(residual * residual, axis=1, keepdims=True)
    first = jnp.sum(gained * table[:ROWS], axis=1, keepdims=True)
    second = jnp.sum(gained * table[ROWS:], axis=1, keepdims=True)
    lane = lax.broadcasted_iota(jnp.int32, (ROWS, HD), 1)
    packed = jnp.where(lane == 0, squares, jnp.where(lane == 1, first, second))
    packed = jnp.concatenate([packed, jnp.zeros((HD - ROWS, HD), jnp.float32)], axis=0)
    sums_ref[...] = jnp.transpose(packed)[:8]


def verdict_kernel(sums_ref, gained_ref, after_ref, hidden_ref, win_ref):
    lines = sums_ref[0]
    for c in range(1, sums_ref.shape[0]):
        lines = lines + sums_ref[c]
    sums = jnp.transpose(lines)[:ROWS]
    inv_rms = 1.0 / jnp.sqrt(sums[:, 0:1] / D + norm_eps)
    hidden_ref[...] = (gained_ref[...] * inv_rms).astype(hidden_ref.dtype)
    inv_rms = 1.0 / jnp.sqrt(lines[0:1] / D + norm_eps)
    win = 1.0 / (1.0 + jnp.exp((lines[2:3] - lines[1:2]) * inv_rms))
    win_ref[...] = win[0, :ROWS]


def attention_kernel(
    lengths_ref, seq_ref, q_hbm, kv_ref, after_ref, out_ref, q_ref, kv_buf, top_ref, total_ref, sum_ref,
    q_sem, sems,
):
    tokens = q_ref.shape[0]
    q_copy = pltpu.make_async_copy(q_hbm, q_ref, q_sem)
    q_copy.start()
    first = seq_ref[0] * tokens
    ends = ends_of(lengths_ref)
    start_first = jnp.int32(0)
    start_last = jnp.int32(0)
    for p in range(PAIRS):
        start_first = jnp.where(ends[p] <= first, ends[p], start_first)
        start_last = jnp.where(ends[p] <= first + tokens - 1, ends[p], start_last)
    low = start_first // KEY_BLOCK
    high = (first + tokens + KEY_BLOCK - 1) // KEY_BLOCK

    def fetch(b):
        rows = pl.ds(pl.multiple_of(b * KEY_BLOCK, KEY_BLOCK), KEY_BLOCK)
        return pltpu.make_async_copy(kv_ref.at[rows], kv_buf.at[rows], sems.at[b])

    def begin(b, carry):
        fetch(b).start()
        return carry

    lax.fori_loop(low, high, begin, 0)
    top_ref[...] = jnp.full_like(top_ref, masked_score)
    total_ref[...] = jnp.zeros_like(total_ref)
    sum_ref[...] = jnp.zeros_like(sum_ref)
    query_pos = lax.broadcasted_iota(jnp.int32, (1, tokens), 1) + first
    query_start = jnp.zeros((1, tokens), jnp.int32)
    for p in range(PAIRS):
        query_start = jnp.where(query_pos >= ends[p], ends[p], query_start)

    def attend(b, masked):
        key_first = b * KEY_BLOCK
        rows = pl.ds(pl.multiple_of(key_first, KEY_BLOCK), KEY_BLOCK)
        keys = kv_buf[rows, :HD]
        values = jnp.transpose(kv_buf[rows, HD:])
        if masked:
            key_pos = lax.broadcasted_iota(jnp.int32, (KEY_BLOCK, tokens), 0) + key_first
            visible = (key_pos >= query_start) & (key_pos <= query_pos)
        for g in range(GROUP):
            queries = q_ref[:, g * HD : (g + 1) * HD]
            scores = lax.dot_general(keys, queries, NT, preferred_element_type=jnp.float32)
            if masked:
                scores = jnp.where(visible, scores, masked_score)
            old_top = top_ref[g]
            tops = jnp.max(scores.reshape(KEY_BLOCK // 8, 8, tokens), axis=0)
            new_top = jnp.maximum(old_top, jnp.max(tops, axis=0, keepdims=True))
            rescale = jnp.exp2((old_top - new_top) * exp2_scale)
            terms = jnp.exp2((scores - new_top) * exp2_scale)
            sums = jnp.sum(terms.reshape(KEY_BLOCK // 8, 8, tokens), axis=0)
            total_ref[g] = total_ref[g] * rescale + sums
            sum_ref[g] = sum_ref[g] * rescale + jnp.dot(
                values, terms.astype(jnp.bfloat16), preferred_element_type=jnp.float32
            )
            top_ref[g] = new_top

    def step(b, carry):
        fetch(b).wait()
        key_first = b * KEY_BLOCK
        masked = (key_first < start_last) | (key_first + KEY_BLOCK > first + 1)

        @pl.when(masked)
        def _():
            attend(b, True)

        @pl.when(jnp.logical_not(masked))
        def _():
            attend(b, False)

        return carry

    q_copy.wait()
    lax.fori_loop(low, high, step, 0)
    for g in range(GROUP):
        total = jnp.sum(total_ref[g], axis=0, keepdims=True)
        rows = jnp.transpose(sum_ref[g] / total)
        out_ref[:, g * HD : (g + 1) * HD] = rows.astype(out_ref.dtype)


def attention(lengths, seq_index, q, kv, after):
    tokens = q.shape[0]
    return pl.pallas_call(
        attention_kernel,
        out_shape=jax.ShapeDtypeStruct(q.shape, q.dtype),
        in_specs=[SM, SM, HB, HB, VM],
        out_specs=VM,
        scratch_shapes=[
            pltpu.VMEM(q.shape, q.dtype),
            pltpu.VMEM(kv.shape, kv.dtype),
            pltpu.VMEM((GROUP, 1, tokens), jnp.float32),
            pltpu.VMEM((GROUP, 8, tokens), jnp.float32),
            pltpu.VMEM((GROUP, HD, tokens), jnp.float32),
            pltpu.SemaphoreType.DMA,
            pltpu.SemaphoreType.DMA((kv.shape[0] // KEY_BLOCK,)),
        ],
        compiler_params=pltpu.CompilerParams(vmem_limit_bytes=24 * 1024 * 1024),
        name="attention",
    )(lengths, seq_index, held(q), held(kv), after)


def call(kernel, shapes, specs, name, scratch=()):
    many = isinstance(shapes, tuple)
    return pl.pallas_call(
        kernel,
        out_shape=shapes,
        in_specs=specs,
        out_specs=tuple(VM for _ in shapes) if many else VM,
        scratch_shapes=list(scratch),
        compiler_params=pltpu.CompilerParams(vmem_limit_bytes=8 * 1024 * 1024),
        name=name,
    )


def shards(
    q_prefill,
    k_prefill,
    v_prefill,
    pair_lengths,
    q_decode,
    cache_k,
    cache_v,
    cache_lengths,
    stream,
    out_weight,
    norm_gain,
    vocab_table,
    verdict_ids,
):
    f32 = jnp.float32
    lo = lax.axis_size("seq_lo")
    hi = lax.axis_size("seq_hi")
    tp = lax.axis_size(TP)
    columns = q_prefill.shape[1]
    width = stream.shape[1]
    pair_lengths, cache_lengths = held(pair_lengths), held(cache_lengths)
    seq_index = lax.axis_index(SEQ).astype(jnp.int32).reshape(1)
    shape = jax.ShapeDtypeStruct

    picked, kv = call(
        last_rows_kernel,
        (
            shape((lo, PAIRS, columns), jnp.bfloat16),
            shape((q_prefill.shape[0], 2 * HD), jnp.bfloat16),
        ),
        [SM, SM, PIPE, PIPE, PIPE],
        "last_rows",
    )(pair_lengths, seq_index, held(q_prefill), held(k_prefill), held(v_prefill))
    kv = lax.all_gather(kv, SEQ, axis=0, tiled=True)
    rows = jnp.sum(exchanged(picked, "seq_lo").astype(f32), axis=0)
    rows = lax.psum(rows.astype(jnp.bfloat16), "seq_hi")

    tp_index = lax.axis_index(TP).astype(jnp.int32).reshape(1)
    hi_index = lax.axis_index("seq_hi").astype(jnp.int32).reshape(1)
    partials, table_rows = call(
        partials_kernel,
        (shape((lo, PART, HD), f32), shape((2 * ROWS, width), f32)),
        [SM] * 5 + [VM] + [PIPE] * 5 + [HB],
        "partials",
        [
            pltpu.VMEM((GROUP * SLOT, HD), f32),
            pltpu.VMEM((2 * ROWS, TABLE_ROWS, width), jnp.bfloat16),
            pltpu.SemaphoreType.DMA((2 * ROWS,)),
        ],
    )(
        pair_lengths, cache_lengths, seq_index, held(verdict_ids.T), tp_index, rows, held(q_decode),
        held(k_prefill), held(v_prefill), held(cache_k), held(cache_v), held(vocab_table),
    )
    slots = call(merge_kernel, shape((hi * PART, HD), jnp.bfloat16), [SM, VM], "merge")(
        hi_index, exchanged(partials, "seq_lo")
    )
    slots = lax.psum(slots, "seq_hi")
    parts = call(finish_kernel, shape((lo, PART, HD), jnp.bfloat16), [VM], "finish")(slots)
    parts = exchanged(parts, "seq_lo")
    pieces = call(
        project_kernel, shape((tp, 3 * ROWS, width), jnp.bfloat16), [VM, PIPE, VM], "project"
    )(parts, held(out_weight), table_rows)
    pieces = exchanged(pieces, TP)
    gained, sums = call(
        residual_kernel,
        (shape((ROWS, width), f32), shape((8, HD), f32)),
        [VM, PIPE, PIPE],
        "residual",
    )(pieces, held(stream), held(norm_gain.reshape(1, width)))
    sums = lax.psum(sums, "seq_hi")
    attended = attention(pair_lengths, seq_index, q_prefill, kv, sums)
    sums = exchanged(jnp.broadcast_to(sums[None], (lo, *sums.shape)), "seq_lo")
    verdict_hidden, win = call(
        verdict_kernel,
        (shape((ROWS, width), jnp.bfloat16), shape((ROWS,), f32)),
        [VM, VM, HB],
        "verdict",
    )(sums, gained, held(attended))

    return (attended, verdict_hidden, win)


def solution(mesh):
    groups, seq = mesh.shape["groups"], mesh.shape["seq"]
    torus = Mesh(
        mesh.devices.reshape(groups, seq // LO, LO, mesh.shape["tp"] // 2, 2),
        ("groups",) + SEQ + TP,
    )
    tokens = ("groups",) + SEQ
    return jax.shard_map(
        shards,
        mesh=torus,
        in_specs=(
            P(tokens, TP),
            P(tokens, TP),
            P(tokens, TP),
            P("groups"),
            P("groups", TP),
            P("groups", SEQ, TP),
            P("groups", SEQ, TP),
            P("groups"),
            P("groups", SEQ),
            P(TP, SEQ),
            P(SEQ),
            P(TP, SEQ),
            P("groups", None),
        ),
        out_specs=(P(tokens, TP), P("groups", SEQ), P("groups")),
        check_vma=False,
    )
```

```python
import functools

import jax
import jax.numpy as jnp
from jax import lax
from jax.experimental import pallas as pl
from jax.experimental.pallas import tpu as pltpu
from jax.sharding import Mesh
from jax.sharding import PartitionSpec as P

D = 8192
H = 32
KVH = 8
HD = 128
PROMPTS = 4
PAIRS = 8
ROWS = 12
GROUP = H // KVH
LO = 8
SLOT = 16
PART = 8
HELD = 6
KEY_BLOCK = 256
TP = ("tp_0", "tp_1")
SEQ = ("seq_hi", "seq_lo")

masked_score = -1e30
norm_eps = 1e-05
score_scale = 1.0 / HD**0.5
exp2_scale = score_scale * 1.4426950408889634

NT = (((1,), (1,)), ((), ()))
VM = pl.BlockSpec(memory_space=pltpu.VMEM)
SM = pl.BlockSpec(memory_space=pltpu.SMEM)
HB = pl.BlockSpec(memory_space=pltpu.HBM)
PIPE = pl.BlockSpec()
TABLE_ROWS = 16


def held(x):
    return pltpu.with_memory_space_constraint(x, pltpu.HBM)


def exchanged(copies, axis):
    return lax.all_to_all(copies, axis, 0, 0, tiled=True)


def ends_of(lengths_ref):
    ends, total = [], 0
    for p in range(PAIRS):
        total = total + lengths_ref[p]
        ends.append(total)
    return ends


def last_rows_kernel(lengths_ref, seq_ref, q_ref, k_ref, v_ref, out_ref, kv_ref):
    kv_ref[:, :HD] = k_ref[...]
    kv_ref[:, HD:] = v_ref[...]
    tokens = q_ref.shape[0]
    ends = ends_of(lengths_ref)
    row = lax.broadcasted_iota(jnp.int32, (SLOT, tokens), 0)
    col = lax.broadcasted_iota(jnp.int32, (SLOT, tokens), 1) + seq_ref[0] * tokens
    last = jnp.full((SLOT, tokens), -1, jnp.int32)
    for p in range(PAIRS):
        last = jnp.where(row == p, ends[p] - 1, last)
    selector = jnp.where(col == last, 1.0, 0.0).astype(jnp.bfloat16)
    picked = jnp.dot(selector, q_ref[...], preferred_element_type=jnp.float32)
    for c in range(out_ref.shape[0]):
        out_ref[c] = picked[:PAIRS].astype(out_ref.dtype)


def table_copies(ids_ref, tp_ref, table_ref, blocks, sems):
    vocab_rows = table_ref.shape[0]
    copies, places = [], []
    for c in range(2):
        for r in range(ROWS):
            local = ids_ref[c, r] - tp_ref[0] * vocab_rows
            inside = (local >= 0) & (local < vocab_rows)
            local = jnp.clip(local, 0, vocab_rows - 1)
            places.append(jnp.where(inside, local % TABLE_ROWS, -1))
            first = pl.multiple_of(local // TABLE_ROWS * TABLE_ROWS, TABLE_ROWS)
            i = len(copies)
            copies.append(
                pltpu.make_async_copy(
                    table_ref.at[pl.ds(first, TABLE_ROWS)], blocks.at[i], sems.at[i]
                )
            )
    return copies, places


def spread(columns):
    row = lax.broadcasted_iota(jnp.int32, (PART, HD), 0)
    lane = lax.broadcasted_iota(jnp.int32, (PART, HD), 1)
    line = jnp.zeros((PART, HD), jnp.float32)
    for j, column in enumerate(columns):
        line = jnp.where(lane == j * PART + row, column, line)
    return jnp.sum(line, axis=0, keepdims=True)


def gathered(line, first, count):
    row = lax.broadcasted_iota(jnp.int32, (PART, HD), 0)
    lane = lax.broadcasted_iota(jnp.int32, (PART, HD), 1)
    wanted = (lane % PART == row) & (lane >= first * PART) & (lane < (first + count) * PART)
    return jnp.sum(jnp.where(wanted, line, 0.0), axis=1, keepdims=True)


def three_parts(x):
    high = x.astype(jnp.bfloat16).astype(jnp.float32)
    middle = (x - high).astype(jnp.bfloat16).astype(jnp.float32)
    return high, middle, x - high - middle


def partials_kernel(
    lengths_ref, cache_lengths_ref, seq_ref, rows_ref, qd_ref, k_ref, v_ref, ck_ref, cv_ref,
    out_ref, q_scratch,
):
    tokens = k_ref.shape[0]
    cache_count = ck_ref.shape[1]
    ends = ends_of(lengths_ref)
    q_scratch[...] = jnp.zeros_like(q_scratch)
    for g in range(GROUP):
        columns = slice(g * HD, (g + 1) * HD)
        base, next_part = g * SLOT, g * SLOT + PART
        both = PAIRS - HELD
        pair_rows = rows_ref[:, columns].astype(jnp.float32)
        q_scratch[base : base + HELD, :] = pair_rows[:HELD]
        q_scratch[next_part : next_part + both, :] = pair_rows[HELD:]
        q_scratch[next_part + both : next_part + HELD, :] = qd_ref[:, columns].astype(jnp.float32)
    queries = q_scratch[...].astype(jnp.bfloat16)
    keys = jnp.concatenate([k_ref[...], ck_ref[...].reshape(PROMPTS * cache_count, HD)], axis=0)
    values = jnp.concatenate([v_ref[...], cv_ref[...].reshape(PROMPTS * cache_count, HD)], axis=0)
    count = tokens + PROMPTS * cache_count
    scores = lax.dot_general(queries, keys, NT, preferred_element_type=jnp.float32) * score_scale
    lane = lax.broadcasted_iota(jnp.int32, (1, count), 1)
    key_pos = lane + seq_ref[0] * tokens
    key_seg = jnp.zeros((1, count), jnp.int32)
    for p in range(PAIRS):
        key_seg = key_seg + jnp.where(key_pos >= ends[p], 1, 0)
    owner = key_seg
    for p in range(PROMPTS):
        first = tokens + p * cache_count
        mine = (lane >= first) & (lane < first + cache_count)
        cache_pos = lane - first + seq_ref[0] * cache_count
        label = jnp.where(cache_pos < cache_lengths_ref[p], PAIRS + p, -1)
        owner = jnp.where(mine, label, owner)
    row = lax.broadcasted_iota(jnp.int32, (GROUP * SLOT, count), 0)
    item = jnp.where(row % PART < HELD, row % PART + row % SLOT // PART * HELD, -2)
    visible = item == owner
    scores = jnp.where(visible, scores, masked_score)
    top = jnp.max(scores, axis=1, keepdims=True)
    terms = jnp.where(visible, jnp.exp(scores - top), 0.0)
    total = jnp.sum(terms, axis=1, keepdims=True)
    sums = jnp.dot(terms.astype(jnp.bfloat16), values, preferred_element_type=jnp.float32)
    place = lax.broadcasted_iota(jnp.int32, (PART, HD), 0)
    for c in range(out_ref.shape[0]):
        rows = slice(c * PART, (c + 1) * PART)
        out_ref[c] = jnp.where(place == HELD, spread((top[rows], total[rows])), sums[rows])


def merged(pieces, parts):
    tops = [gathered(piece[HELD : HELD + 1], 0, parts) for piece in pieces]
    totals = [gathered(piece[HELD : HELD + 1], parts, parts) for piece in pieces]
    top = functools.reduce(jnp.maximum, tops)
    total = jnp.zeros_like(top)
    sums = jnp.zeros((PART, HD), jnp.float32)
    for piece, piece_top, piece_total in zip(pieces, tops, totals):
        scale = jnp.exp(piece_top - top)
        total = total + piece_total * scale
        sums = sums + piece * scale
    return sums, top, total


def merge_kernel(hi_ref, pieces_ref, out_ref):
    sums, top, total = merged([pieces_ref[c] for c in range(pieces_ref.shape[0])], 1)
    row = lax.broadcasted_iota(jnp.int32, (PART, HD), 0)
    line = spread(three_parts(top) + three_parts(total))
    block = jnp.where(row == HELD, line, jnp.where(row < HELD, sums, 0.0))
    slots = [jnp.where(hi_ref[0] == k, block, 0.0) for k in range(out_ref.shape[0] // PART)]
    out_ref[...] = jnp.concatenate(slots, axis=0).astype(out_ref.dtype)


def finish_kernel(slots_ref, out_ref):
    slots = slots_ref[...].astype(jnp.float32)
    count = slots_ref.shape[0] // PART
    sums, _, total = merged([slots[k * PART : (k + 1) * PART] for k in range(count)], 3)
    row = lax.broadcasted_iota(jnp.int32, (PART, HD), 0)
    rows = jnp.where(row < HELD, sums / total, 0.0).astype(out_ref.dtype)
    for c in range(out_ref.shape[0]):
        out_ref[c] = rows


def prepare_kernel(
    ids_ref, tp_ref, after_ref, w_hbm, table_ref, picked_ref, w_ref, blocks, w_sem, sems
):
    copies, places = table_copies(ids_ref, tp_ref, table_ref, blocks, sems)
    w_copy = pltpu.make_async_copy(w_hbm, w_ref, w_sem)
    for copy in copies:
        copy.start()
    w_copy.start()
    for copy in copies:
        copy.wait()
    index = lax.broadcasted_iota(jnp.int32, blocks.shape[1:], 0)
    for i, wanted in enumerate(places):
        block = jnp.where(index == wanted, blocks[i].astype(jnp.float32), 0.0)
        picked_ref[i : i + 1, :] = jnp.sum(block, axis=0, keepdims=True)
    w_copy.wait()


def project_kernel(parts_ref, w_ref, table_ref, out_ref):
    partial = jnp.zeros((SLOT, w_ref.shape[1]), jnp.float32)
    for g in range(GROUP):
        rows = [parts_ref[2 * g + j].astype(jnp.float32) for j in range(2)]
        partial = partial + jnp.dot(
            jnp.concatenate(rows, axis=0).astype(jnp.bfloat16),
            w_ref[g * HD : (g + 1) * HD, :],
            preferred_element_type=jnp.float32,
        )
    both = jnp.concatenate(
        [partial[:HELD], partial[PART : PART + HELD], table_ref[...]], axis=0
    ).astype(out_ref.dtype)
    for c in range(out_ref.shape[0]):
        out_ref[c] = both


def residual_kernel(pieces_ref, stream_ref, gain_ref, gained_ref, sums_ref):
    total = pieces_ref[0].astype(jnp.float32)
    for c in range(1, pieces_ref.shape[0]):
        total = total + pieces_ref[c].astype(jnp.float32)
    table = total[ROWS:]
    residual = total[:ROWS] + stream_ref[...].astype(jnp.float32)
    gained = residual * gain_ref[...].astype(jnp.float32)
    gained_ref[...] = gained
    squares = jnp.sum(residual * residual, axis=1, keepdims=True)
    first = jnp.sum(gained * table[:ROWS], axis=1, keepdims=True)
    second = jnp.sum(gained * table[ROWS:], axis=1, keepdims=True)
    lane = lax.broadcasted_iota(jnp.int32, (ROWS, HD), 1)
    packed = jnp.where(lane == 0, squares, jnp.where(lane == 1, first, second))
    packed = jnp.concatenate([packed, jnp.zeros((HD - ROWS, HD), jnp.float32)], axis=0)
    sums_ref[...] = jnp.transpose(packed)[:8]


def verdict_kernel(sums_ref, gained_ref, after_ref, hidden_ref, win_ref):
    lines = sums_ref[0]
    for c in range(1, sums_ref.shape[0]):
        lines = lines + sums_ref[c]
    sums = jnp.transpose(lines)[:ROWS]
    inv_rms = 1.0 / jnp.sqrt(sums[:, 0:1] / D + norm_eps)
    hidden_ref[...] = (gained_ref[...] * inv_rms).astype(hidden_ref.dtype)
    inv_rms = 1.0 / jnp.sqrt(lines[0:1] / D + norm_eps)
    win = 1.0 / (1.0 + jnp.exp((lines[2:3] - lines[1:2]) * inv_rms))
    win_ref[...] = win[0, :ROWS]


def attention_kernel(
    lengths_ref, seq_ref, q_hbm, kv_ref, after_ref, out_ref, q_ref, kv_buf, top_ref, total_ref, sum_ref,
    q_sem, sems,
):
    tokens = q_ref.shape[0]
    q_copy = pltpu.make_async_copy(q_hbm, q_ref, q_sem)
    q_copy.start()
    first = seq_ref[0] * tokens
    ends = ends_of(lengths_ref)
    start_first = jnp.int32(0)
    start_last = jnp.int32(0)
    for p in range(PAIRS):
        start_first = jnp.where(ends[p] <= first, ends[p], start_first)
        start_last = jnp.where(ends[p] <= first + tokens - 1, ends[p], start_last)
    low = start_first // KEY_BLOCK
    high = (first + tokens + KEY_BLOCK - 1) // KEY_BLOCK

    def fetch(b):
        rows = pl.ds(pl.multiple_of(b * KEY_BLOCK, KEY_BLOCK), KEY_BLOCK)
        return pltpu.make_async_copy(kv_ref.at[rows], kv_buf.at[rows], sems.at[b])

    def begin(b, carry):
        fetch(b).start()
        return carry

    lax.fori_loop(low, high, begin, 0)
    top_ref[...] = jnp.full_like(top_ref, masked_score)
    total_ref[...] = jnp.zeros_like(total_ref)
    sum_ref[...] = jnp.zeros_like(sum_ref)
    query_pos = lax.broadcasted_iota(jnp.int32, (1, tokens), 1) + first
    query_start = jnp.zeros((1, tokens), jnp.int32)
    for p in range(PAIRS):
        query_start = jnp.where(query_pos >= ends[p], ends[p], query_start)

    def attend(b, masked):
        key_first = b * KEY_BLOCK
        rows = pl.ds(pl.multiple_of(key_first, KEY_BLOCK), KEY_BLOCK)
        keys = kv_buf[rows, :HD]
        values = jnp.transpose(kv_buf[rows, HD:])
        if masked:
            key_pos = lax.broadcasted_iota(jnp.int32, (KEY_BLOCK, tokens), 0) + key_first
            visible = (key_pos >= query_start) & (key_pos <= query_pos)
        for g in range(GROUP):
            queries = q_ref[:, g * HD : (g + 1) * HD]
            scores = lax.dot_general(keys, queries, NT, preferred_element_type=jnp.float32)
            if masked:
                scores = jnp.where(visible, scores, masked_score)
            old_top = top_ref[g]
            tops = jnp.max(scores.reshape(KEY_BLOCK // 8, 8, tokens), axis=0)
            new_top = jnp.maximum(old_top, jnp.max(tops, axis=0, keepdims=True))
            rescale = jnp.exp2((old_top - new_top) * exp2_scale)
            terms = jnp.exp2((scores - new_top) * exp2_scale)
            sums = jnp.sum(terms.reshape(KEY_BLOCK // 8, 8, tokens), axis=0)
            total_ref[g] = total_ref[g] * rescale + sums
            sum_ref[g] = sum_ref[g] * rescale + jnp.dot(
                values, terms.astype(jnp.bfloat16), preferred_element_type=jnp.float32
            )
            top_ref[g] = new_top

    def step(b, carry):
        fetch(b).wait()
        key_first = b * KEY_BLOCK
        masked = (key_first < start_last) | (key_first + KEY_BLOCK > first + 1)

        @pl.when(masked)
        def _():
            attend(b, True)

        @pl.when(jnp.logical_not(masked))
        def _():
            attend(b, False)

        return carry

    q_copy.wait()
    lax.fori_loop(low, high, step, 0)
    for g in range(GROUP):
        total = jnp.sum(total_ref[g], axis=0, keepdims=True)
        rows = jnp.transpose(sum_ref[g] / total)
        out_ref[:, g * HD : (g + 1) * HD] = rows.astype(out_ref.dtype)


def attention(lengths, seq_index, q, kv, after):
    tokens = q.shape[0]
    return pl.pallas_call(
        attention_kernel,
        out_shape=jax.ShapeDtypeStruct(q.shape, q.dtype),
        in_specs=[SM, SM, HB, HB, VM],
        out_specs=VM,
        scratch_shapes=[
            pltpu.VMEM(q.shape, q.dtype),
            pltpu.VMEM(kv.shape, kv.dtype),
            pltpu.VMEM((GROUP, 1, tokens), jnp.float32),
            pltpu.VMEM((GROUP, 8, tokens), jnp.float32),
            pltpu.VMEM((GROUP, HD, tokens), jnp.float32),
            pltpu.SemaphoreType.DMA,
            pltpu.SemaphoreType.DMA((kv.shape[0] // KEY_BLOCK,)),
        ],
        compiler_params=pltpu.CompilerParams(vmem_limit_bytes=24 * 1024 * 1024),
        name="attention",
    )(lengths, seq_index, held(q), held(kv), after)


def call(kernel, shapes, specs, name, scratch=()):
    many = isinstance(shapes, tuple)
    return pl.pallas_call(
        kernel,
        out_shape=shapes,
        in_specs=specs,
        out_specs=tuple(VM for _ in shapes) if many else VM,
        scratch_shapes=list(scratch),
        compiler_params=pltpu.CompilerParams(vmem_limit_bytes=8 * 1024 * 1024),
        name=name,
    )


def shards(
    q_prefill,
    k_prefill,
    v_prefill,
    pair_lengths,
    q_decode,
    cache_k,
    cache_v,
    cache_lengths,
    stream,
    out_weight,
    norm_gain,
    vocab_table,
    verdict_ids,
):
    f32 = jnp.float32
    lo = lax.axis_size("seq_lo")
    hi = lax.axis_size("seq_hi")
    tp = lax.axis_size(TP)
    columns = q_prefill.shape[1]
    width = stream.shape[1]
    pair_lengths, cache_lengths = held(pair_lengths), held(cache_lengths)
    seq_index = lax.axis_index(SEQ).astype(jnp.int32).reshape(1)
    shape = jax.ShapeDtypeStruct

    picked, kv = call(
        last_rows_kernel,
        (
            shape((lo, PAIRS, columns), jnp.bfloat16),
            shape((q_prefill.shape[0], 2 * HD), jnp.bfloat16),
        ),
        [SM, SM, PIPE, PIPE, PIPE],
        "last_rows",
    )(pair_lengths, seq_index, held(q_prefill), held(k_prefill), held(v_prefill))
    kv = lax.all_gather(kv, SEQ, axis=0, tiled=True)
    rows = jnp.sum(exchanged(picked, "seq_lo").astype(f32), axis=0)
    rows = lax.psum(rows.astype(jnp.bfloat16), "seq_hi")

    tp_index = lax.axis_index(TP).astype(jnp.int32).reshape(1)
    hi_index = lax.axis_index("seq_hi").astype(jnp.int32).reshape(1)
    partials = call(
        partials_kernel,
        shape((lo, PART, HD), f32),
        [SM] * 3 + [VM] + [PIPE] * 5,
        "partials",
        [pltpu.VMEM((GROUP * SLOT, HD), f32)],
    )(
        pair_lengths, cache_lengths, seq_index, rows, held(q_decode), held(k_prefill),
        held(v_prefill), held(cache_k), held(cache_v),
    )
    slots = call(merge_kernel, shape((hi * PART, HD), jnp.bfloat16), [SM, VM], "merge")(
        hi_index, exchanged(partials, "seq_lo")
    )
    slots = lax.psum(slots, "seq_hi")
    parts = call(finish_kernel, shape((lo, PART, HD), jnp.bfloat16), [VM], "finish")(slots)
    table_rows, weight = call(
        prepare_kernel,
        (shape((2 * ROWS, width), f32), shape(out_weight.shape, out_weight.dtype)),
        [SM, SM, VM, HB, HB],
        "prepare",
        [
            pltpu.VMEM((2 * ROWS, TABLE_ROWS, width), jnp.bfloat16),
            pltpu.SemaphoreType.DMA,
            pltpu.SemaphoreType.DMA((2 * ROWS,)),
        ],
    )(held(verdict_ids.T), tp_index, parts, held(out_weight), held(vocab_table))
    parts = exchanged(parts, "seq_lo")
    pieces = call(
        project_kernel, shape((tp, 3 * ROWS, width), jnp.bfloat16), [VM, VM, VM], "project"
    )(parts, weight, table_rows)
    pieces = exchanged(pieces, TP)
    gained, sums = call(
        residual_kernel,
        (shape((ROWS, width), f32), shape((8, HD), f32)),
        [VM, PIPE, PIPE],
        "residual",
    )(pieces, held(stream), held(norm_gain.reshape(1, width)))
    sums = lax.psum(sums, "seq_hi")
    attended = attention(pair_lengths, seq_index, q_prefill, kv, sums)
    sums = exchanged(jnp.broadcast_to(sums[None], (lo, *sums.shape)), "seq_lo")
    verdict_hidden, win = call(
        verdict_kernel,
        (shape((ROWS, width), jnp.bfloat16), shape((ROWS,), f32)),
        [VM, VM, HB],
        "verdict",
    )(sums, gained, held(attended))

    return (attended, verdict_hidden, win)


def solution(mesh):
    groups, seq = mesh.shape["groups"], mesh.shape["seq"]
    torus = Mesh(
        mesh.devices.reshape(groups, seq // LO, LO, mesh.shape["tp"] // 2, 2),
        ("groups",) + SEQ + TP,
    )
    tokens = ("groups",) + SEQ
    return jax.shard_map(
        shards,
        mesh=torus,
        in_specs=(
            P(tokens, TP),
            P(tokens, TP),
            P(tokens, TP),
            P("groups"),
            P("groups", TP),
            P("groups", SEQ, TP),
            P("groups", SEQ, TP),
            P("groups"),
            P("groups", SEQ),
            P(TP, SEQ),
            P(SEQ),
            P(TP, SEQ),
            P("groups", None),
        ),
        out_specs=(P(tokens, TP), P("groups", SEQ), P("groups")),
        check_vma=False,
    )
```

```python
import functools

import jax
import jax.numpy as jnp
from jax import lax
from jax.experimental import pallas as pl
from jax.experimental.pallas import tpu as pltpu
from jax.sharding import Mesh
from jax.sharding import PartitionSpec as P

D = 8192
H = 32
KVH = 8
HD = 128
PROMPTS = 4
PAIRS = 8
ROWS = 12
GROUP = H // KVH
LO = 8
SLOT = 16
PART = 8
HELD = 6
KEY_BLOCK = 256
TP = ("tp_0", "tp_1")
SEQ = ("seq_hi", "seq_lo")

masked_score = -1e30
norm_eps = 1e-05
score_scale = 1.0 / HD**0.5
exp2_scale = score_scale * 1.4426950408889634

NT = (((1,), (1,)), ((), ()))
VM = pl.BlockSpec(memory_space=pltpu.VMEM)
SM = pl.BlockSpec(memory_space=pltpu.SMEM)
HB = pl.BlockSpec(memory_space=pltpu.HBM)
PIPE = pl.BlockSpec()
TABLE_ROWS = 16


def held(x):
    return pltpu.with_memory_space_constraint(x, pltpu.HBM)


def exchanged(copies, axis):
    return lax.all_to_all(copies, axis, 0, 0, tiled=True)


def ends_of(lengths_ref):
    ends, total = [], 0
    for p in range(PAIRS):
        total = total + lengths_ref[p]
        ends.append(total)
    return ends


def last_rows_kernel(lengths_ref, seq_ref, q_ref, k_ref, v_ref, out_ref, kv_ref):
    kv_ref[:, :HD] = k_ref[...]
    kv_ref[:, HD:] = v_ref[...]
    tokens = q_ref.shape[0]
    ends = ends_of(lengths_ref)
    row = lax.broadcasted_iota(jnp.int32, (SLOT, tokens), 0)
    col = lax.broadcasted_iota(jnp.int32, (SLOT, tokens), 1) + seq_ref[0] * tokens
    last = jnp.full((SLOT, tokens), -1, jnp.int32)
    for p in range(PAIRS):
        last = jnp.where(row == p, ends[p] - 1, last)
    selector = jnp.where(col == last, 1.0, 0.0).astype(jnp.bfloat16)
    picked = jnp.dot(selector, q_ref[...], preferred_element_type=jnp.float32)
    for c in range(out_ref.shape[0]):
        out_ref[c] = picked[:PAIRS].astype(out_ref.dtype)


def table_copies(ids_ref, tp_ref, table_ref, blocks, sems):
    vocab_rows = table_ref.shape[0]
    copies, places = [], []
    for c in range(2):
        for r in range(ROWS):
            local = ids_ref[c, r] - tp_ref[0] * vocab_rows
            inside = (local >= 0) & (local < vocab_rows)
            local = jnp.clip(local, 0, vocab_rows - 1)
            places.append(jnp.where(inside, local % TABLE_ROWS, -1))
            first = pl.multiple_of(local // TABLE_ROWS * TABLE_ROWS, TABLE_ROWS)
            i = len(copies)
            copies.append(
                pltpu.make_async_copy(
                    table_ref.at[pl.ds(first, TABLE_ROWS)], blocks.at[i], sems.at[i]
                )
            )
    return copies, places


def spread(columns):
    row = lax.broadcasted_iota(jnp.int32, (PART, HD), 0)
    lane = lax.broadcasted_iota(jnp.int32, (PART, HD), 1)
    line = jnp.zeros((PART, HD), jnp.float32)
    for j, column in enumerate(columns):
        line = jnp.where(lane == j * PART + row, column, line)
    return jnp.sum(line, axis=0, keepdims=True)


def gathered(line, first, count):
    row = lax.broadcasted_iota(jnp.int32, (PART, HD), 0)
    lane = lax.broadcasted_iota(jnp.int32, (PART, HD), 1)
    wanted = (lane % PART == row) & (lane >= first * PART) & (lane < (first + count) * PART)
    return jnp.sum(jnp.where(wanted, line, 0.0), axis=1, keepdims=True)


def three_parts(x):
    high = x.astype(jnp.bfloat16).astype(jnp.float32)
    middle = (x - high).astype(jnp.bfloat16).astype(jnp.float32)
    return high, middle, x - high - middle


def partials_kernel(
    lengths_ref, cache_lengths_ref, seq_ref, rows_ref, qd_ref, k_ref, v_ref, ck_ref, cv_ref,
    after_ref, out_ref, q_scratch,
):
    tokens = k_ref.shape[0]
    cache_count = ck_ref.shape[1]
    ends = ends_of(lengths_ref)
    q_scratch[...] = jnp.zeros_like(q_scratch)
    for g in range(GROUP):
        columns = slice(g * HD, (g + 1) * HD)
        base, next_part = g * SLOT, g * SLOT + PART
        both = PAIRS - HELD
        pair_rows = rows_ref[:, columns].astype(jnp.float32)
        q_scratch[base : base + HELD, :] = pair_rows[:HELD]
        q_scratch[next_part : next_part + both, :] = pair_rows[HELD:]
        q_scratch[next_part + both : next_part + HELD, :] = qd_ref[:, columns].astype(jnp.float32)
    queries = q_scratch[...].astype(jnp.bfloat16)
    keys = jnp.concatenate([k_ref[...], ck_ref[...].reshape(PROMPTS * cache_count, HD)], axis=0)
    values = jnp.concatenate([v_ref[...], cv_ref[...].reshape(PROMPTS * cache_count, HD)], axis=0)
    count = tokens + PROMPTS * cache_count
    scores = lax.dot_general(queries, keys, NT, preferred_element_type=jnp.float32) * score_scale
    lane = lax.broadcasted_iota(jnp.int32, (1, count), 1)
    key_pos = lane + seq_ref[0] * tokens
    key_seg = jnp.zeros((1, count), jnp.int32)
    for p in range(PAIRS):
        key_seg = key_seg + jnp.where(key_pos >= ends[p], 1, 0)
    owner = key_seg
    for p in range(PROMPTS):
        first = tokens + p * cache_count
        mine = (lane >= first) & (lane < first + cache_count)
        cache_pos = lane - first + seq_ref[0] * cache_count
        label = jnp.where(cache_pos < cache_lengths_ref[p], PAIRS + p, -1)
        owner = jnp.where(mine, label, owner)
    row = lax.broadcasted_iota(jnp.int32, (GROUP * SLOT, count), 0)
    item = jnp.where(row % PART < HELD, row % PART + row % SLOT // PART * HELD, -2)
    visible = item == owner
    scores = jnp.where(visible, scores, masked_score)
    top = jnp.max(scores, axis=1, keepdims=True)
    terms = jnp.where(visible, jnp.exp(scores - top), 0.0)
    total = jnp.sum(terms, axis=1, keepdims=True)
    sums = jnp.dot(terms.astype(jnp.bfloat16), values, preferred_element_type=jnp.float32)
    place = lax.broadcasted_iota(jnp.int32, (PART, HD), 0)
    for c in range(out_ref.shape[0]):
        rows = slice(c * PART, (c + 1) * PART)
        out_ref[c] = jnp.where(place == HELD, spread((top[rows], total[rows])), sums[rows])


def merged(pieces, parts):
    tops = [gathered(piece[HELD : HELD + 1], 0, parts) for piece in pieces]
    totals = [gathered(piece[HELD : HELD + 1], parts, parts) for piece in pieces]
    top = functools.reduce(jnp.maximum, tops)
    total = jnp.zeros_like(top)
    sums = jnp.zeros((PART, HD), jnp.float32)
    for piece, piece_top, piece_total in zip(pieces, tops, totals):
        scale = jnp.exp(piece_top - top)
        total = total + piece_total * scale
        sums = sums + piece * scale
    return sums, top, total


def merge_kernel(hi_ref, pieces_ref, out_ref):
    sums, top, total = merged([pieces_ref[c] for c in range(pieces_ref.shape[0])], 1)
    row = lax.broadcasted_iota(jnp.int32, (PART, HD), 0)
    line = spread(three_parts(top) + three_parts(total))
    block = jnp.where(row == HELD, line, jnp.where(row < HELD, sums, 0.0))
    slots = [jnp.where(hi_ref[0] == k, block, 0.0) for k in range(out_ref.shape[0] // PART)]
    out_ref[...] = jnp.concatenate(slots, axis=0).astype(out_ref.dtype)


def finish_kernel(slots_ref, out_ref):
    slots = slots_ref[...].astype(jnp.float32)
    count = slots_ref.shape[0] // PART
    sums, _, total = merged([slots[k * PART : (k + 1) * PART] for k in range(count)], 3)
    row = lax.broadcasted_iota(jnp.int32, (PART, HD), 0)
    rows = jnp.where(row < HELD, sums / total, 0.0).astype(out_ref.dtype)
    for c in range(out_ref.shape[0]):
        out_ref[c] = rows


def table_kernel(ids_ref, tp_ref, after_ref, table_ref, picked_ref, blocks, sems):
    copies, places = table_copies(ids_ref, tp_ref, table_ref, blocks, sems)
    for copy in copies:
        copy.start()
    for copy in copies:
        copy.wait()
    index = lax.broadcasted_iota(jnp.int32, blocks.shape[1:], 0)
    for i, wanted in enumerate(places):
        block = jnp.where(index == wanted, blocks[i].astype(jnp.float32), 0.0)
        picked_ref[i : i + 1, :] = jnp.sum(block, axis=0, keepdims=True)


def weight_kernel(after_ref, w_hbm, w_ref, w_sem):
    w_copy = pltpu.make_async_copy(w_hbm, w_ref, w_sem)
    w_copy.start()
    w_copy.wait()


def project_kernel(parts_ref, w_ref, table_ref, out_ref):
    partial = jnp.zeros((SLOT, w_ref.shape[1]), jnp.float32)
    for g in range(GROUP):
        rows = [parts_ref[2 * g + j].astype(jnp.float32) for j in range(2)]
        partial = partial + jnp.dot(
            jnp.concatenate(rows, axis=0).astype(jnp.bfloat16),
            w_ref[g * HD : (g + 1) * HD, :],
            preferred_element_type=jnp.float32,
        )
    both = jnp.concatenate(
        [partial[:HELD], partial[PART : PART + HELD], table_ref[...]], axis=0
    ).astype(out_ref.dtype)
    for c in range(out_ref.shape[0]):
        out_ref[c] = both


def residual_kernel(pieces_ref, stream_ref, gain_ref, gained_ref, sums_ref):
    total = pieces_ref[0].astype(jnp.float32)
    for c in range(1, pieces_ref.shape[0]):
        total = total + pieces_ref[c].astype(jnp.float32)
    table = total[ROWS:]
    residual = total[:ROWS] + stream_ref[...].astype(jnp.float32)
    gained = residual * gain_ref[...].astype(jnp.float32)
    gained_ref[...] = gained
    squares = jnp.sum(residual * residual, axis=1, keepdims=True)
    first = jnp.sum(gained * table[:ROWS], axis=1, keepdims=True)
    second = jnp.sum(gained * table[ROWS:], axis=1, keepdims=True)
    lane = lax.broadcasted_iota(jnp.int32, (ROWS, HD), 1)
    packed = jnp.where(lane == 0, squares, jnp.where(lane == 1, first, second))
    packed = jnp.concatenate([packed, jnp.zeros((HD - ROWS, HD), jnp.float32)], axis=0)
    sums_ref[...] = jnp.transpose(packed)[:8]


def verdict_kernel(sums_ref, gained_ref, after_ref, hidden_ref, win_ref):
    lines = sums_ref[0]
    for c in range(1, sums_ref.shape[0]):
        lines = lines + sums_ref[c]
    sums = jnp.transpose(lines)[:ROWS]
    inv_rms = 1.0 / jnp.sqrt(sums[:, 0:1] / D + norm_eps)
    hidden_ref[...] = (gained_ref[...] * inv_rms).astype(hidden_ref.dtype)
    inv_rms = 1.0 / jnp.sqrt(lines[0:1] / D + norm_eps)
    win = 1.0 / (1.0 + jnp.exp((lines[2:3] - lines[1:2]) * inv_rms))
    win_ref[...] = win[0, :ROWS]


def attention_kernel(
    lengths_ref, seq_ref, q_hbm, kv_ref, after_ref, out_ref, q_ref, kv_buf, top_ref, total_ref, sum_ref,
    q_sem, sems,
):
    tokens = q_ref.shape[0]
    q_copy = pltpu.make_async_copy(q_hbm, q_ref, q_sem)
    q_copy.start()
    first = seq_ref[0] * tokens
    ends = ends_of(lengths_ref)
    start_first = jnp.int32(0)
    start_last = jnp.int32(0)
    for p in range(PAIRS):
        start_first = jnp.where(ends[p] <= first, ends[p], start_first)
        start_last = jnp.where(ends[p] <= first + tokens - 1, ends[p], start_last)
    low = start_first // KEY_BLOCK
    high = (first + tokens + KEY_BLOCK - 1) // KEY_BLOCK

    def fetch(b):
        rows = pl.ds(pl.multiple_of(b * KEY_BLOCK, KEY_BLOCK), KEY_BLOCK)
        return pltpu.make_async_copy(kv_ref.at[rows], kv_buf.at[rows], sems.at[b])

    def begin(b, carry):
        fetch(b).start()
        return carry

    lax.fori_loop(low, high, begin, 0)
    top_ref[...] = jnp.full_like(top_ref, masked_score)
    total_ref[...] = jnp.zeros_like(total_ref)
    sum_ref[...] = jnp.zeros_like(sum_ref)
    query_pos = lax.broadcasted_iota(jnp.int32, (1, tokens), 1) + first
    query_start = jnp.zeros((1, tokens), jnp.int32)
    for p in range(PAIRS):
        query_start = jnp.where(query_pos >= ends[p], ends[p], query_start)

    def attend(b, masked):
        key_first = b * KEY_BLOCK
        rows = pl.ds(pl.multiple_of(key_first, KEY_BLOCK), KEY_BLOCK)
        keys = kv_buf[rows, :HD]
        values = jnp.transpose(kv_buf[rows, HD:])
        if masked:
            key_pos = lax.broadcasted_iota(jnp.int32, (KEY_BLOCK, tokens), 0) + key_first
            visible = (key_pos >= query_start) & (key_pos <= query_pos)
        for g in range(GROUP):
            queries = q_ref[:, g * HD : (g + 1) * HD]
            scores = lax.dot_general(keys, queries, NT, preferred_element_type=jnp.float32)
            if masked:
                scores = jnp.where(visible, scores, masked_score)
            old_top = top_ref[g]
            tops = jnp.max(scores.reshape(KEY_BLOCK // 8, 8, tokens), axis=0)
            new_top = jnp.maximum(old_top, jnp.max(tops, axis=0, keepdims=True))
            rescale = jnp.exp2((old_top - new_top) * exp2_scale)
            terms = jnp.exp2((scores - new_top) * exp2_scale)
            sums = jnp.sum(terms.reshape(KEY_BLOCK // 8, 8, tokens), axis=0)
            total_ref[g] = total_ref[g] * rescale + sums
            sum_ref[g] = sum_ref[g] * rescale + jnp.dot(
                values, terms.astype(jnp.bfloat16), preferred_element_type=jnp.float32
            )
            top_ref[g] = new_top

    def step(b, carry):
        fetch(b).wait()
        key_first = b * KEY_BLOCK
        masked = (key_first < start_last) | (key_first + KEY_BLOCK > first + 1)

        @pl.when(masked)
        def _():
            attend(b, True)

        @pl.when(jnp.logical_not(masked))
        def _():
            attend(b, False)

        return carry

    q_copy.wait()
    lax.fori_loop(low, high, step, 0)
    for g in range(GROUP):
        total = jnp.sum(total_ref[g], axis=0, keepdims=True)
        rows = jnp.transpose(sum_ref[g] / total)
        out_ref[:, g * HD : (g + 1) * HD] = rows.astype(out_ref.dtype)


def attention(lengths, seq_index, q, kv, after):
    tokens = q.shape[0]
    return pl.pallas_call(
        attention_kernel,
        out_shape=jax.ShapeDtypeStruct(q.shape, q.dtype),
        in_specs=[SM, SM, HB, HB, VM],
        out_specs=VM,
        scratch_shapes=[
            pltpu.VMEM(q.shape, q.dtype),
            pltpu.VMEM(kv.shape, kv.dtype),
            pltpu.VMEM((GROUP, 1, tokens), jnp.float32),
            pltpu.VMEM((GROUP, 8, tokens), jnp.float32),
            pltpu.VMEM((GROUP, HD, tokens), jnp.float32),
            pltpu.SemaphoreType.DMA,
            pltpu.SemaphoreType.DMA((kv.shape[0] // KEY_BLOCK,)),
        ],
        compiler_params=pltpu.CompilerParams(vmem_limit_bytes=24 * 1024 * 1024),
        name="attention",
    )(lengths, seq_index, held(q), held(kv), after)


def call(kernel, shapes, specs, name, scratch=()):
    many = isinstance(shapes, tuple)
    return pl.pallas_call(
        kernel,
        out_shape=shapes,
        in_specs=specs,
        out_specs=tuple(VM for _ in shapes) if many else VM,
        scratch_shapes=list(scratch),
        compiler_params=pltpu.CompilerParams(vmem_limit_bytes=8 * 1024 * 1024),
        name=name,
    )


def shards(
    q_prefill,
    k_prefill,
    v_prefill,
    pair_lengths,
    q_decode,
    cache_k,
    cache_v,
    cache_lengths,
    stream,
    out_weight,
    norm_gain,
    vocab_table,
    verdict_ids,
):
    f32 = jnp.float32
    lo = lax.axis_size("seq_lo")
    hi = lax.axis_size("seq_hi")
    tp = lax.axis_size(TP)
    columns = q_prefill.shape[1]
    width = stream.shape[1]
    pair_lengths, cache_lengths = held(pair_lengths), held(cache_lengths)
    seq_index = lax.axis_index(SEQ).astype(jnp.int32).reshape(1)
    shape = jax.ShapeDtypeStruct

    picked, kv = call(
        last_rows_kernel,
        (
            shape((lo, PAIRS, columns), jnp.bfloat16),
            shape((q_prefill.shape[0], 2 * HD), jnp.bfloat16),
        ),
        [SM, SM, PIPE, PIPE, PIPE],
        "last_rows",
    )(pair_lengths, seq_index, held(q_prefill), held(k_prefill), held(v_prefill))
    kv = lax.all_gather(kv, SEQ, axis=0, tiled=True)
    tp_index = lax.axis_index(TP).astype(jnp.int32).reshape(1)
    table_rows = call(
        table_kernel,
        shape((2 * ROWS, width), f32),
        [SM, SM, HB, HB],
        "table",
        [
            pltpu.VMEM((2 * ROWS, TABLE_ROWS, width), jnp.bfloat16),
            pltpu.SemaphoreType.DMA((2 * ROWS,)),
        ],
    )(held(verdict_ids.T), tp_index, picked, held(vocab_table))
    table_rows = held(table_rows)
    rows = jnp.sum(exchanged(picked, "seq_lo").astype(f32), axis=0)
    rows = lax.psum(rows.astype(jnp.bfloat16), "seq_hi")

    hi_index = lax.axis_index("seq_hi").astype(jnp.int32).reshape(1)
    partials = call(
        partials_kernel,
        shape((lo, PART, HD), f32),
        [SM] * 3 + [VM] + [PIPE] * 5 + [HB],
        "partials",
        [pltpu.VMEM((GROUP * SLOT, HD), f32)],
    )(
        pair_lengths, cache_lengths, seq_index, rows, held(q_decode), held(k_prefill),
        held(v_prefill), held(cache_k), held(cache_v), table_rows,
    )
    slots = call(merge_kernel, shape((hi * PART, HD), jnp.bfloat16), [SM, VM], "merge")(
        hi_index, exchanged(partials, "seq_lo")
    )
    slots = lax.psum(slots, "seq_hi")
    parts = call(finish_kernel, shape((lo, PART, HD), jnp.bfloat16), [VM], "finish")(slots)
    weight = call(
        weight_kernel,
        shape(out_weight.shape, out_weight.dtype),
        [VM, HB],
        "weight",
        [pltpu.SemaphoreType.DMA],
    )(parts, held(out_weight))
    parts = exchanged(parts, "seq_lo")
    pieces = call(
        project_kernel, shape((tp, 3 * ROWS, width), jnp.bfloat16), [VM, VM, PIPE], "project"
    )(parts, weight, table_rows)
    pieces = exchanged(pieces, TP)
    gained, sums = call(
        residual_kernel,
        (shape((ROWS, width), f32), shape((8, HD), f32)),
        [VM, PIPE, PIPE],
        "residual",
    )(pieces, held(stream), held(norm_gain.reshape(1, width)))
    sums = lax.psum(sums, "seq_hi")
    attended = attention(pair_lengths, seq_index, q_prefill, kv, sums)
    sums = exchanged(jnp.broadcast_to(sums[None], (lo, *sums.shape)), "seq_lo")
    verdict_hidden, win = call(
        verdict_kernel,
        (shape((ROWS, width), jnp.bfloat16), shape((ROWS,), f32)),
        [VM, VM, HB],
        "verdict",
    )(sums, gained, held(attended))

    return (attended, verdict_hidden, win)


def solution(mesh):
    groups, seq = mesh.shape["groups"], mesh.shape["seq"]
    torus = Mesh(
        mesh.devices.reshape(groups, seq // LO, LO, mesh.shape["tp"] // 2, 2),
        ("groups",) + SEQ + TP,
    )
    tokens = ("groups",) + SEQ
    return jax.shard_map(
        shards,
        mesh=torus,
        in_specs=(
            P(tokens, TP),
            P(tokens, TP),
            P(tokens, TP),
            P("groups"),
            P("groups", TP),
            P("groups", SEQ, TP),
            P("groups", SEQ, TP),
            P("groups"),
            P("groups", SEQ),
            P(TP, SEQ),
            P(SEQ),
            P(TP, SEQ),
            P("groups", None),
        ),
        out_specs=(P(tokens, TP), P("groups", SEQ), P("groups")),
        check_vma=False,
    )
```

```python
import functools

import jax
import jax.numpy as jnp
from jax import lax
from jax.experimental import pallas as pl
from jax.experimental.pallas import tpu as pltpu
from jax.sharding import Mesh
from jax.sharding import PartitionSpec as P

D = 8192
H = 32
KVH = 8
HD = 128
PROMPTS = 4
PAIRS = 8
ROWS = 12
GROUP = H // KVH
LO = 8
SLOT = 16
PART = 8
HELD = 6
KEY_BLOCK = 512
TP = ("tp_0", "tp_1")
SEQ = ("seq_hi", "seq_lo")

masked_score = -1e30
norm_eps = 1e-05
score_scale = 1.0 / HD**0.5
exp2_scale = score_scale * 1.4426950408889634

NT = (((1,), (1,)), ((), ()))
VM = pl.BlockSpec(memory_space=pltpu.VMEM)
SM = pl.BlockSpec(memory_space=pltpu.SMEM)
HB = pl.BlockSpec(memory_space=pltpu.HBM)
PIPE = pl.BlockSpec()
TABLE_ROWS = 16


def held(x):
    return pltpu.with_memory_space_constraint(x, pltpu.HBM)


def exchanged(copies, axis):
    return lax.all_to_all(copies, axis, 0, 0, tiled=True)


def ends_of(lengths_ref):
    ends, total = [], 0
    for p in range(PAIRS):
        total = total + lengths_ref[p]
        ends.append(total)
    return ends


def last_rows_kernel(lengths_ref, seq_ref, q_ref, k_ref, v_ref, out_ref, kv_ref):
    kv_ref[:, :HD] = k_ref[...]
    kv_ref[:, HD:] = v_ref[...]
    tokens = q_ref.shape[0]
    ends = ends_of(lengths_ref)
    row = lax.broadcasted_iota(jnp.int32, (SLOT, tokens), 0)
    col = lax.broadcasted_iota(jnp.int32, (SLOT, tokens), 1) + seq_ref[0] * tokens
    last = jnp.full((SLOT, tokens), -1, jnp.int32)
    for p in range(PAIRS):
        last = jnp.where(row == p, ends[p] - 1, last)
    selector = jnp.where(col == last, 1.0, 0.0).astype(jnp.bfloat16)
    picked = jnp.dot(selector, q_ref[...], preferred_element_type=jnp.float32)
    for c in range(out_ref.shape[0]):
        out_ref[c] = picked[:PAIRS].astype(out_ref.dtype)


def table_copies(ids_ref, tp_ref, table_ref, blocks, sems):
    vocab_rows = table_ref.shape[0]
    copies, places = [], []
    for c in range(2):
        for r in range(ROWS):
            local = ids_ref[c, r] - tp_ref[0] * vocab_rows
            inside = (local >= 0) & (local < vocab_rows)
            local = jnp.clip(local, 0, vocab_rows - 1)
            places.append(jnp.where(inside, local % TABLE_ROWS, -1))
            first = pl.multiple_of(local // TABLE_ROWS * TABLE_ROWS, TABLE_ROWS)
            i = len(copies)
            copies.append(
                pltpu.make_async_copy(
                    table_ref.at[pl.ds(first, TABLE_ROWS)], blocks.at[i], sems.at[i]
                )
            )
    return copies, places


def spread(columns):
    row = lax.broadcasted_iota(jnp.int32, (PART, HD), 0)
    lane = lax.broadcasted_iota(jnp.int32, (PART, HD), 1)
    line = jnp.zeros((PART, HD), jnp.float32)
    for j, column in enumerate(columns):
        line = jnp.where(lane == j * PART + row, column, line)
    return jnp.sum(line, axis=0, keepdims=True)


def gathered(line, first, count):
    row = lax.broadcasted_iota(jnp.int32, (PART, HD), 0)
    lane = lax.broadcasted_iota(jnp.int32, (PART, HD), 1)
    wanted = (lane % PART == row) & (lane >= first * PART) & (lane < (first + count) * PART)
    return jnp.sum(jnp.where(wanted, line, 0.0), axis=1, keepdims=True)


def three_parts(x):
    high = x.astype(jnp.bfloat16).astype(jnp.float32)
    middle = (x - high).astype(jnp.bfloat16).astype(jnp.float32)
    return high, middle, x - high - middle


def partials_kernel(
    lengths_ref, cache_lengths_ref, seq_ref, rows_ref, qd_ref, k_ref, v_ref, ck_ref, cv_ref,
    out_ref, q_scratch,
):
    tokens = k_ref.shape[0]
    cache_count = ck_ref.shape[1]
    ends = ends_of(lengths_ref)
    q_scratch[...] = jnp.zeros_like(q_scratch)
    for g in range(GROUP):
        columns = slice(g * HD, (g + 1) * HD)
        base, next_part = g * SLOT, g * SLOT + PART
        both = PAIRS - HELD
        pair_rows = rows_ref[:, columns].astype(jnp.float32)
        q_scratch[base : base + HELD, :] = pair_rows[:HELD]
        q_scratch[next_part : next_part + both, :] = pair_rows[HELD:]
        q_scratch[next_part + both : next_part + HELD, :] = qd_ref[:, columns].astype(jnp.float32)
    queries = q_scratch[...].astype(jnp.bfloat16)
    keys = jnp.concatenate([k_ref[...], ck_ref[...].reshape(PROMPTS * cache_count, HD)], axis=0)
    values = jnp.concatenate([v_ref[...], cv_ref[...].reshape(PROMPTS * cache_count, HD)], axis=0)
    count = tokens + PROMPTS * cache_count
    scores = lax.dot_general(queries, keys, NT, preferred_element_type=jnp.float32) * score_scale
    lane = lax.broadcasted_iota(jnp.int32, (1, count), 1)
    key_pos = lane + seq_ref[0] * tokens
    key_seg = jnp.zeros((1, count), jnp.int32)
    for p in range(PAIRS):
        key_seg = key_seg + jnp.where(key_pos >= ends[p], 1, 0)
    owner = key_seg
    for p in range(PROMPTS):
        first = tokens + p * cache_count
        mine = (lane >= first) & (lane < first + cache_count)
        cache_pos = lane - first + seq_ref[0] * cache_count
        label = jnp.where(cache_pos < cache_lengths_ref[p], PAIRS + p, -1)
        owner = jnp.where(mine, label, owner)
    row = lax.broadcasted_iota(jnp.int32, (GROUP * SLOT, count), 0)
    item = jnp.where(row % PART < HELD, row % PART + row % SLOT // PART * HELD, -2)
    visible = item == owner
    scores = jnp.where(visible, scores, masked_score)
    top = jnp.max(scores, axis=1, keepdims=True)
    terms = jnp.where(visible, jnp.exp(scores - top), 0.0)
    total = jnp.sum(terms, axis=1, keepdims=True)
    sums = jnp.dot(terms.astype(jnp.bfloat16), values, preferred_element_type=jnp.float32)
    place = lax.broadcasted_iota(jnp.int32, (PART, HD), 0)
    for c in range(out_ref.shape[0]):
        rows = slice(c * PART, (c + 1) * PART)
        out_ref[c] = jnp.where(place == HELD, spread((top[rows], total[rows])), sums[rows])


def merged(pieces, parts):
    tops = [gathered(piece[HELD : HELD + 1], 0, parts) for piece in pieces]
    totals = [gathered(piece[HELD : HELD + 1], parts, parts) for piece in pieces]
    top = functools.reduce(jnp.maximum, tops)
    total = jnp.zeros_like(top)
    sums = jnp.zeros((PART, HD), jnp.float32)
    for piece, piece_top, piece_total in zip(pieces, tops, totals):
        scale = jnp.exp(piece_top - top)
        total = total + piece_total * scale
        sums = sums + piece * scale
    return sums, top, total


def merge_kernel(hi_ref, pieces_ref, out_ref):
    sums, top, total = merged([pieces_ref[c] for c in range(pieces_ref.shape[0])], 1)
    row = lax.broadcasted_iota(jnp.int32, (PART, HD), 0)
    line = spread(three_parts(top) + three_parts(total))
    block = jnp.where(row == HELD, line, jnp.where(row < HELD, sums, 0.0))
    slots = [jnp.where(hi_ref[0] == k, block, 0.0) for k in range(out_ref.shape[0] // PART)]
    out_ref[...] = jnp.concatenate(slots, axis=0).astype(out_ref.dtype)


def finish_kernel(slots_ref, out_ref):
    slots = slots_ref[...].astype(jnp.float32)
    count = slots_ref.shape[0] // PART
    sums, _, total = merged([slots[k * PART : (k + 1) * PART] for k in range(count)], 3)
    row = lax.broadcasted_iota(jnp.int32, (PART, HD), 0)
    rows = jnp.where(row < HELD, sums / total, 0.0).astype(out_ref.dtype)
    for c in range(out_ref.shape[0]):
        out_ref[c] = rows


def prepare_kernel(
    ids_ref, tp_ref, after_ref, w_hbm, table_ref, picked_ref, w_ref, blocks, w_sem, sems
):
    copies, places = table_copies(ids_ref, tp_ref, table_ref, blocks, sems)
    w_copy = pltpu.make_async_copy(w_hbm, w_ref, w_sem)
    for copy in copies:
        copy.start()
    w_copy.start()
    for copy in copies:
        copy.wait()
    index = lax.broadcasted_iota(jnp.int32, blocks.shape[1:], 0)
    for i, wanted in enumerate(places):
        block = jnp.where(index == wanted, blocks[i].astype(jnp.float32), 0.0)
        picked_ref[i : i + 1, :] = jnp.sum(block, axis=0, keepdims=True)
    w_copy.wait()


def project_kernel(parts_ref, w_ref, table_ref, out_ref):
    partial = jnp.zeros((SLOT, w_ref.shape[1]), jnp.float32)
    for g in range(GROUP):
        rows = [parts_ref[2 * g + j].astype(jnp.float32) for j in range(2)]
        partial = partial + jnp.dot(
            jnp.concatenate(rows, axis=0).astype(jnp.bfloat16),
            w_ref[g * HD : (g + 1) * HD, :],
            preferred_element_type=jnp.float32,
        )
    both = jnp.concatenate(
        [partial[:HELD], partial[PART : PART + HELD], table_ref[...]], axis=0
    ).astype(out_ref.dtype)
    for c in range(out_ref.shape[0]):
        out_ref[c] = both


def residual_kernel(pieces_ref, stream_ref, gain_ref, gained_ref, sums_ref):
    total = pieces_ref[0].astype(jnp.float32)
    for c in range(1, pieces_ref.shape[0]):
        total = total + pieces_ref[c].astype(jnp.float32)
    table = total[ROWS:]
    residual = total[:ROWS] + stream_ref[...].astype(jnp.float32)
    gained = residual * gain_ref[...].astype(jnp.float32)
    gained_ref[...] = gained
    squares = jnp.sum(residual * residual, axis=1, keepdims=True)
    first = jnp.sum(gained * table[:ROWS], axis=1, keepdims=True)
    second = jnp.sum(gained * table[ROWS:], axis=1, keepdims=True)
    lane = lax.broadcasted_iota(jnp.int32, (ROWS, HD), 1)
    packed = jnp.where(lane == 0, squares, jnp.where(lane == 1, first, second))
    packed = jnp.concatenate([packed, jnp.zeros((HD - ROWS, HD), jnp.float32)], axis=0)
    sums_ref[...] = jnp.transpose(packed)[:8]


def verdict_kernel(sums_ref, gained_ref, after_ref, hidden_ref, win_ref):
    lines = sums_ref[0]
    for c in range(1, sums_ref.shape[0]):
        lines = lines + sums_ref[c]
    sums = jnp.transpose(lines)[:ROWS]
    inv_rms = 1.0 / jnp.sqrt(sums[:, 0:1] / D + norm_eps)
    hidden_ref[...] = (gained_ref[...] * inv_rms).astype(hidden_ref.dtype)
    inv_rms = 1.0 / jnp.sqrt(lines[0:1] / D + norm_eps)
    win = 1.0 / (1.0 + jnp.exp((lines[2:3] - lines[1:2]) * inv_rms))
    win_ref[...] = win[0, :ROWS]


def attention_kernel(
    lengths_ref, seq_ref, q_hbm, kv_ref, after_ref, out_ref, q_ref, kv_buf, top_ref, total_ref, sum_ref,
    q_sem, sems,
):
    tokens = q_ref.shape[0]
    q_copy = pltpu.make_async_copy(q_hbm, q_ref, q_sem)
    q_copy.start()
    first = seq_ref[0] * tokens
    ends = ends_of(lengths_ref)
    start_first = jnp.int32(0)
    start_last = jnp.int32(0)
    for p in range(PAIRS):
        start_first = jnp.where(ends[p] <= first, ends[p], start_first)
        start_last = jnp.where(ends[p] <= first + tokens - 1, ends[p], start_last)
    low = start_first // KEY_BLOCK
    high = (first + tokens + KEY_BLOCK - 1) // KEY_BLOCK

    def fetch(b):
        rows = pl.ds(pl.multiple_of(b * KEY_BLOCK, KEY_BLOCK), KEY_BLOCK)
        return pltpu.make_async_copy(kv_ref.at[rows], kv_buf.at[rows], sems.at[b])

    def begin(b, carry):
        fetch(b).start()
        return carry

    lax.fori_loop(low, high, begin, 0)
    top_ref[...] = jnp.full_like(top_ref, masked_score)
    total_ref[...] = jnp.zeros_like(total_ref)
    sum_ref[...] = jnp.zeros_like(sum_ref)
    query_pos = lax.broadcasted_iota(jnp.int32, (1, tokens), 1) + first
    query_start = jnp.zeros((1, tokens), jnp.int32)
    for p in range(PAIRS):
        query_start = jnp.where(query_pos >= ends[p], ends[p], query_start)

    def attend(b, masked):
        key_first = b * KEY_BLOCK
        rows = pl.ds(pl.multiple_of(key_first, KEY_BLOCK), KEY_BLOCK)
        keys = kv_buf[rows, :HD]
        values = jnp.transpose(kv_buf[rows, HD:])
        if masked:
            key_pos = lax.broadcasted_iota(jnp.int32, (KEY_BLOCK, tokens), 0) + key_first
            visible = (key_pos >= query_start) & (key_pos <= query_pos)
        for g in range(GROUP):
            queries = q_ref[:, g * HD : (g + 1) * HD]
            scores = lax.dot_general(keys, queries, NT, preferred_element_type=jnp.float32)
            if masked:
                scores = jnp.where(visible, scores, masked_score)
            old_top = top_ref[g]
            tops = jnp.max(scores.reshape(KEY_BLOCK // 8, 8, tokens), axis=0)
            new_top = jnp.maximum(old_top, jnp.max(tops, axis=0, keepdims=True))
            rescale = jnp.exp2((old_top - new_top) * exp2_scale)
            terms = jnp.exp2((scores - new_top) * exp2_scale)
            sums = jnp.sum(terms.reshape(KEY_BLOCK // 8, 8, tokens), axis=0)
            total_ref[g] = total_ref[g] * rescale + sums
            sum_ref[g] = sum_ref[g] * rescale + jnp.dot(
                values, terms.astype(jnp.bfloat16), preferred_element_type=jnp.float32
            )
            top_ref[g] = new_top

    def step(b, carry):
        fetch(b).wait()
        key_first = b * KEY_BLOCK
        masked = (key_first < start_last) | (key_first + KEY_BLOCK > first + 1)

        @pl.when(masked)
        def _():
            attend(b, True)

        @pl.when(jnp.logical_not(masked))
        def _():
            attend(b, False)

        return carry

    q_copy.wait()
    lax.fori_loop(low, high, step, 0)
    for g in range(GROUP):
        total = jnp.sum(total_ref[g], axis=0, keepdims=True)
        rows = jnp.transpose(sum_ref[g] / total)
        out_ref[:, g * HD : (g + 1) * HD] = rows.astype(out_ref.dtype)


def attention(lengths, seq_index, q, kv, after):
    tokens = q.shape[0]
    return pl.pallas_call(
        attention_kernel,
        out_shape=jax.ShapeDtypeStruct(q.shape, q.dtype),
        in_specs=[SM, SM, HB, HB, VM],
        out_specs=VM,
        scratch_shapes=[
            pltpu.VMEM(q.shape, q.dtype),
            pltpu.VMEM(kv.shape, kv.dtype),
            pltpu.VMEM((GROUP, 1, tokens), jnp.float32),
            pltpu.VMEM((GROUP, 8, tokens), jnp.float32),
            pltpu.VMEM((GROUP, HD, tokens), jnp.float32),
            pltpu.SemaphoreType.DMA,
            pltpu.SemaphoreType.DMA((kv.shape[0] // KEY_BLOCK,)),
        ],
        compiler_params=pltpu.CompilerParams(vmem_limit_bytes=24 * 1024 * 1024),
        name="attention",
    )(lengths, seq_index, held(q), held(kv), after)


def call(kernel, shapes, specs, name, scratch=()):
    many = isinstance(shapes, tuple)
    return pl.pallas_call(
        kernel,
        out_shape=shapes,
        in_specs=specs,
        out_specs=tuple(VM for _ in shapes) if many else VM,
        scratch_shapes=list(scratch),
        compiler_params=pltpu.CompilerParams(vmem_limit_bytes=8 * 1024 * 1024),
        name=name,
    )


def shards(
    q_prefill,
    k_prefill,
    v_prefill,
    pair_lengths,
    q_decode,
    cache_k,
    cache_v,
    cache_lengths,
    stream,
    out_weight,
    norm_gain,
    vocab_table,
    verdict_ids,
):
    f32 = jnp.float32
    lo = lax.axis_size("seq_lo")
    hi = lax.axis_size("seq_hi")
    tp = lax.axis_size(TP)
    columns = q_prefill.shape[1]
    width = stream.shape[1]
    pair_lengths, cache_lengths = held(pair_lengths), held(cache_lengths)
    seq_index = lax.axis_index(SEQ).astype(jnp.int32).reshape(1)
    shape = jax.ShapeDtypeStruct

    picked, kv = call(
        last_rows_kernel,
        (
            shape((lo, PAIRS, columns), jnp.bfloat16),
            shape((q_prefill.shape[0], 2 * HD), jnp.bfloat16),
        ),
        [SM, SM, PIPE, PIPE, PIPE],
        "last_rows",
    )(pair_lengths, seq_index, held(q_prefill), held(k_prefill), held(v_prefill))
    kv = lax.all_gather(kv, SEQ, axis=0, tiled=True)
    rows = jnp.sum(exchanged(picked, "seq_lo").astype(f32), axis=0)
    rows = lax.psum(rows.astype(jnp.bfloat16), "seq_hi")

    tp_index = lax.axis_index(TP).astype(jnp.int32).reshape(1)
    hi_index = lax.axis_index("seq_hi").astype(jnp.int32).reshape(1)
    partials = call(
        partials_kernel,
        shape((lo, PART, HD), f32),
        [SM] * 3 + [VM] + [PIPE] * 5,
        "partials",
        [pltpu.VMEM((GROUP * SLOT, HD), f32)],
    )(
        pair_lengths, cache_lengths, seq_index, rows, held(q_decode), held(k_prefill),
        held(v_prefill), held(cache_k), held(cache_v),
    )
    slots = call(merge_kernel, shape((hi * PART, HD), jnp.bfloat16), [SM, VM], "merge")(
        hi_index, exchanged(partials, "seq_lo")
    )
    slots = lax.psum(slots, "seq_hi")
    parts = call(finish_kernel, shape((lo, PART, HD), jnp.bfloat16), [VM], "finish")(slots)
    table_rows, weight = call(
        prepare_kernel,
        (shape((2 * ROWS, width), f32), shape(out_weight.shape, out_weight.dtype)),
        [SM, SM, VM, HB, HB],
        "prepare",
        [
            pltpu.VMEM((2 * ROWS, TABLE_ROWS, width), jnp.bfloat16),
            pltpu.SemaphoreType.DMA,
            pltpu.SemaphoreType.DMA((2 * ROWS,)),
        ],
    )(held(verdict_ids.T), tp_index, parts, held(out_weight), held(vocab_table))
    parts = exchanged(parts, "seq_lo")
    pieces = call(
        project_kernel, shape((tp, 3 * ROWS, width), jnp.bfloat16), [VM, VM, VM], "project"
    )(parts, weight, table_rows)
    pieces = exchanged(pieces, TP)
    gained, sums = call(
        residual_kernel,
        (shape((ROWS, width), f32), shape((8, HD), f32)),
        [VM, PIPE, PIPE],
        "residual",
    )(pieces, held(stream), held(norm_gain.reshape(1, width)))
    sums = lax.psum(sums, "seq_hi")
    attended = attention(pair_lengths, seq_index, q_prefill, kv, sums)
    sums = exchanged(jnp.broadcast_to(sums[None], (lo, *sums.shape)), "seq_lo")
    verdict_hidden, win = call(
        verdict_kernel,
        (shape((ROWS, width), jnp.bfloat16), shape((ROWS,), f32)),
        [VM, VM, HB],
        "verdict",
    )(sums, gained, held(attended))

    return (attended, verdict_hidden, win)


def solution(mesh):
    groups, seq = mesh.shape["groups"], mesh.shape["seq"]
    torus = Mesh(
        mesh.devices.reshape(groups, seq // LO, LO, mesh.shape["tp"] // 2, 2),
        ("groups",) + SEQ + TP,
    )
    tokens = ("groups",) + SEQ
    return jax.shard_map(
        shards,
        mesh=torus,
        in_specs=(
            P(tokens, TP),
            P(tokens, TP),
            P(tokens, TP),
            P("groups"),
            P("groups", TP),
            P("groups", SEQ, TP),
            P("groups", SEQ, TP),
            P("groups"),
            P("groups", SEQ),
            P(TP, SEQ),
            P(SEQ),
            P(TP, SEQ),
            P("groups", None),
        ),
        out_specs=(P(tokens, TP), P("groups", SEQ), P("groups")),
        check_vma=False,
    )
```
